256 devices in a mesh: dp: 16 (over z_lo, x, core), tensor: 16 (over z_hi, y).
Axes of the slice: x: 4, y: 4, z: 8 (z_hi: 4, z_lo: 2; z = z_hi * 2 + z_lo), core: 2. Of those that a mesh axis runs over, the one named last changes fastest.
Arguments:
- activations: bfloat16 [4096, 5120], P('dp'), may hold values from -6 to 6
- grad_out: bfloat16 [4096, 5120], P('dp'), may hold values from -6 to 6
- gate_pre: bfloat16 [4096, 7168], P('dp', 'tensor'), may hold values from -8 to 8
- up_pre: bfloat16 [4096, 7168], P('dp', 'tensor'), may hold values from -6 to 6
- gate_up: bfloat16 [5120, 2, 7168], P('dp', None, 'tensor'), may hold values from -0.078125 to 0.078125
- down_weight: bfloat16 [5120, 7168], P('dp', 'tensor'), may hold values from -0.0625 to 0.0625
Outputs:
- grad_input: bfloat16 [4096, 5120], P('dp')
- grad_gate_up: float32 [5120, 2, 7168], P('dp', None, 'tensor')
- grad_down: float32 [5120, 7168], P('dp', 'tensor')
The draws below stay inside these ranges and needn't reach their ends.
All inputs are finite; a program needn't handle non-finite values.
Results may differ from the reference program's by a relative error of at most 0.017.
Values may be sent and summed in bfloat16 or wider, within the bound.
No kernel may reach another device: no remote copies, remote signals or barrier semaphores. Data moves between devices by JAX's collectives and lax.ppermute only.
A program may use at most 128 MiB of HBM per device.

```python
import jax
import jax.numpy as jnp
from jax import lax

D = 5120
FF = 7168
TOK_DEV = 256
TOKENS = 4096
N_DP = 16
N_TENSOR = 16


def raised(result, stream_key, source, target, blocks, factor):
    owner, partner = [(jnp.arange(result.shape[dim]) // (result.shape[dim] // blocks)).reshape([-1 if axis == dim else 1 for axis in range(result.ndim)]) for dim in (source, target)]
    chosen = jax.random.permutation(stream_key, blocks)[partner]
    strong = (owner == chosen) | (owner == (partner + blocks // 2) % blocks)
    return jnp.where(strong, factor * result, result)


def shard_levels(own_key, extent, cuts, low, high):
    def one(dim, shards_of):
        draws = jax.random.uniform(jax.random.fold_in(jax.random.fold_in(own_key, 6), dim), (shards_of,), jnp.float32, low / len(cuts), high / len(cuts))
        return jnp.repeat(jnp.exp(draws), extent[dim] // shards_of).reshape((-1,) + (1,) * (len(extent) - dim - 1))

    gain = one(*cuts[0])
    for cut in cuts[1:]:
        gain = gain * one(*cut)
    return gain


def scatter_about(own_key, dims, scale, bound, shards=(), kind=jnp.bfloat16):
    array = jax.random.normal(own_key, dims, jnp.float32) * scale
    if len(shards) > 0:
        array = shard_levels(own_key, dims, shards, -0.22, 0.18) * array
    return jnp.clip(array, min=-bound, max=bound).astype(kind)


def gaussian_with(key, shape, scale, bound, split, heavy, kind=jnp.bfloat16):
    drawn = scale * jax.random.normal(key, shape, jnp.float32)
    if split:
        drawn = drawn * shard_levels(key, shape, split, -0.22, 0.18)
    return jnp.clip(raised(drawn, jax.random.fold_in(key, 3), *heavy), -bound, bound).astype(kind)


def setup_inputs(seed: int = 0) -> dict:
    key_list = jax.random.split(jax.random.key(seed), 7)
    return {
        "activations": gaussian_with(key_list[0], (TOKENS, D), 1.0, 6.0, ((0, 16),), (0, 1, 16, 2.0)),
        "grad_out": gaussian_with(key_list[1], (TOKENS, D), 1.0, 6.0, ((0, 16),), (0, 1, 16, 2.0)),
        "gate_pre": scatter_about(key_list[2], (TOKENS, FF), 1.5, 8.0, ((0, 16), (1, 16))),
        "up_pre": scatter_about(key_list[3], (TOKENS, FF), 1.0, 6.0, ((0, 16), (1, 16))),
        "gate_up": scatter_about(key_list[4], (D, 2, FF), D ** -0.5, 0.078125, ((0, 16), (2, 16))),
        "down_weight": scatter_about(key_list[5], (D, FF), FF ** -0.5, 0.0625, ((0, 16), (1, 16))),
    }


def reference(activations, grad_out, gate_pre, up_pre, gate_up, down_weight):
    gate_wide = gate_pre.astype(jnp.float32)
    up_wide = up_pre.astype(jnp.float32)
    gate_sigmoid = jax.nn.sigmoid(gate_wide)
    gate_silu = gate_wide * gate_sigmoid
    hidden = (gate_silu * up_wide).astype(jnp.bfloat16)
    grad_h = jnp.dot(grad_out, down_weight, preferred_element_type=jnp.float32)
    grad_gate = grad_h * up_wide * gate_sigmoid * (1.0 + gate_wide * (1.0 - gate_sigmoid))
    grad_up = grad_h * gate_silu
    grad_hidden = jnp.stack([grad_gate, grad_up], axis=1).astype(jnp.bfloat16)

    group_width = FF // N_TENSOR
    hidden_groups = grad_hidden.reshape(TOKENS, 2, N_TENSOR, group_width).transpose(2, 0, 1, 3)
    hidden_groups = hidden_groups.reshape(N_TENSOR, TOKENS, 2 * group_width)
    weight_groups = gate_up.reshape(D, 2, N_TENSOR, group_width).transpose(2, 0, 1, 3)
    weight_groups = weight_groups.reshape(N_TENSOR, D, 2 * group_width)

    def add_part(running, paired):
        left_rows, right_rows = paired
        part_sum = jnp.dot(left_rows, right_rows.T, preferred_element_type=jnp.float32)
        part_sum = lax.optimization_barrier(part_sum.astype(jnp.bfloat16))
        return running + part_sum.astype(jnp.float32), None

    input_total, _ = lax.scan(add_part, jnp.zeros((TOKENS, D), jnp.float32), (hidden_groups, weight_groups))
    grad_input = input_total.astype(jnp.bfloat16)

    act_groups = activations.reshape(N_DP, TOK_DEV, D)
    out_groups = grad_out.reshape(N_DP, TOK_DEV, D)
    grad_groups = grad_hidden.reshape(N_DP, TOK_DEV, 2 * FF)
    plain_groups = hidden.reshape(N_DP, TOK_DEV, FF)

    def add_group(running, group_items):
        act_rows, out_rows, grad_rows, plain_rows = group_items
        gate_part = jnp.dot(act_rows.T, grad_rows, preferred_element_type=jnp.float32)
        down_part = jnp.dot(out_rows.T, plain_rows, preferred_element_type=jnp.float32)
        gate_part = lax.optimization_barrier(gate_part.astype(jnp.bfloat16))
        down_part = lax.optimization_barrier(down_part.astype(jnp.bfloat16))
        return (running[0] + gate_part.astype(jnp.float32), running[1] + down_part.astype(jnp.float32)), None

    start_sums = (jnp.zeros((D, 2 * FF), jnp.float32), jnp.zeros((D, FF), jnp.float32))
    summed, _ = lax.scan(add_group, start_sums, (act_groups, out_groups, grad_groups, plain_groups))
    grad_gate_up = (summed[0] / N_DP).reshape(D, 2, FF)
    grad_down = summed[1] / N_DP
    return grad_input, grad_gate_up, grad_down
```

```python
import jax
import jax.numpy as jnp
from jax import lax
from jax.experimental import pallas as pl
from jax.experimental.pallas import tpu as pltpu
from jax.sharding import Mesh
from jax.sharding import PartitionSpec as P

Z, X, C = "dp_0", "dp_1", "dp_2"
DP = (Z, X, C)
ZH, Y = "tensor_0", "tensor_1"
TENSOR = (ZH, Y)
BF = jnp.bfloat16
F32 = jnp.float32


def shift(v, axis, step):
    n = lax.axis_size(axis)
    return lax.ppermute(v, axis, [(i, (i + step) % n) for i in range(n)])


def to_slabs_kernel(pos_ref, x_ref, mine_ref, theirs_ref, *, slab, nx):
    z_odd = pos_ref[0] == 1
    core_odd = pos_ref[1] == 1
    for xx in range(nx):
        q = pos_ref[2 + xx]
        cols = []
        for zz in range(2):
            k = zz * nx + xx
            even = x_ref[:, (2 * k) * slab : (2 * k + 1) * slab]
            odd = x_ref[:, (2 * k + 1) * slab : (2 * k + 2) * slab]
            cols.append((jnp.where(core_odd, odd, even), jnp.where(core_odd, even, odd)))
        for ref, i in ((mine_ref, 0), (theirs_ref, 1)):
            near = jnp.where(z_odd, cols[1][i], cols[0][i])
            far = jnp.where(z_odd, cols[0][i], cols[1][i])
            ref[q] = jnp.concatenate([near, far], axis=1)


def to_slabs(x, pos, slab, nx):
    tokens, width = x.shape
    rows = 64
    out = jax.ShapeDtypeStruct((nx, tokens, 2 * slab), x.dtype)
    import functools

    return pl.pallas_call(
        functools.partial(to_slabs_kernel, slab=slab, nx=nx),
        grid_spec=pltpu.PrefetchScalarGridSpec(
            num_scalar_prefetch=1,
            grid=(tokens // rows,),
            in_specs=[pl.BlockSpec((rows, width), lambda i, s: (i, 0))],
            out_specs=[pl.BlockSpec((nx, rows, 2 * slab), lambda i, s: (0, i, 0))] * 2,
        ),
        out_shape=[out, out],
        name="to_slabs",
    )(pos, x)


def from_slabs_kernel(pos_ref, *refs, slab, nx):
    own_refs, other_refs, o_ref = refs[:nx], refs[nx : 2 * nx], refs[-1]
    z_odd = pos_ref[0] == 1
    core_odd = pos_ref[1] == 1
    shift_by = pos_ref[2]

    def placed(rs):
        v = [r[...] for r in rs]
        for s in (1, 2):
            on = (shift_by & s) != 0
            v = [jnp.where(on, v[(i - s) % nx], v[i]) for i in range(nx)]
        return v

    own, other = placed(own_refs), placed(other_refs)
    for xx in range(nx):
        halves = []
        for v in (own, other):
            near, far = v[xx][:, :slab], v[xx][:, slab:]
            halves.append((jnp.where(z_odd, far, near), jnp.where(z_odd, near, far)))
        for zz in range(2):
            k = zz * nx + xx
            mine, theirs = halves[0][zz], halves[1][zz]
            even = jnp.where(core_odd, theirs, mine)
            odd = jnp.where(core_odd, mine, theirs)
            o_ref[:, 2 * k * slab : (2 * k + 2) * slab] = jnp.concatenate([even, odd], axis=1)


def from_slabs(own, other, pos, slab):
    nx = len(own)
    rows = own[0].shape[0]
    import functools

    return pl.pallas_call(
        functools.partial(from_slabs_kernel, slab=slab, nx=nx),
        in_specs=[pl.BlockSpec(memory_space=pltpu.SMEM)]
        + [pl.BlockSpec(memory_space=pltpu.VMEM)] * (2 * nx),
        out_shape=jax.ShapeDtypeStruct((rows, 4 * nx * slab), own[0].dtype),
        name="from_slabs",
    )(pos, *own, *other)


def gather_pairs(s):
    rows = s.shape[0]
    right = shift(s, X, 1)
    left = shift(s, X, -1)
    b = shift(s, Z, 1)
    b_right = shift(b, X, 1)
    b_left = shift(b, X, -1)
    two_a = shift(right, X, 1)
    two_b = shift(b_left, X, -1)
    return {
        0: jnp.concatenate([s, b]),
        3: jnp.concatenate([right, b_right]),
        1: jnp.concatenate([left, b_left]),
        2: jnp.concatenate([two_a, two_b]),
    }


def scatter_pairs(make):
    p2 = make(2)
    half = p2.shape[0] // 2
    r_plus = shift(p2[:half].astype(BF), X, 1)
    r_minus = shift(p2[half:].astype(BF), X, -1)
    p1 = make(1)
    p3 = make(3)
    far_from_left = shift(p1[half:].astype(BF), X, 1)
    near_from_right = shift(p3[:half].astype(BF), X, -1)
    near_from_left = shift((p1[:half] + r_plus.astype(F32)).astype(BF), X, 1)
    far_from_right = shift((p3[half:] + r_minus.astype(F32)).astype(BF), X, -1)
    p0 = make(0)
    far = p0[half:] + far_from_left.astype(F32) + far_from_right.astype(F32)
    got = shift(far.astype(BF), Z, 1)
    near = p0[:half] + near_from_left.astype(F32) + near_from_right.astype(F32)
    return near + got.astype(F32)


def per_device(activations, grad_out, gate_pre, up_pre, gate_up, down_weight):
    tokens = activations.shape[0]
    slab, width = down_weight.shape
    nx, ny, nz = lax.axis_size(X), lax.axis_size(Y), lax.axis_size(ZH)
    dp_count = lax.axis_size(DP)
    xi, zi, ci = lax.axis_index(X), lax.axis_index(Z), lax.axis_index(C)
    yi, zh = lax.axis_index(Y), lax.axis_index(ZH)
    pos = jnp.stack([zi, ci] + [(k - xi) % nx for k in range(nx)]).astype(jnp.int32)
    pos_back = jnp.stack([zi, ci, xi]).astype(jnp.int32)

    down = gather_pairs(down_weight)
    gate_flat = gate_up.reshape(slab, 2 * width)
    gates = gather_pairs(gate_flat)

    out_mine, out_theirs = to_slabs(grad_out, pos, slab, nx)
    out_all = jnp.concatenate([out_mine, shift(out_theirs, C, 1)], axis=1)
    act_mine, act_theirs = to_slabs(activations, pos, slab, nx)
    act_all = jnp.concatenate([act_mine, shift(act_theirs, C, 1)], axis=1)
    gate_all = jnp.concatenate([gate_pre, shift(gate_pre, C, 1)]).astype(F32)
    up_all = jnp.concatenate([up_pre, shift(up_pre, C, 1)]).astype(F32)

    gate_sigmoid = jax.nn.sigmoid(gate_all)
    gate_silu = gate_all * gate_sigmoid
    hidden = (gate_silu * up_all).astype(BF)

    part_h = sum(
        jnp.dot(out_all[q], down[q], preferred_element_type=F32) for q in (0, 1, 3, 2)
    )
    got_h = shift(part_h, C, 1)
    grad_h = part_h + jnp.concatenate([got_h[tokens:], got_h[:tokens]])
    grad_gate = grad_h * up_all * gate_sigmoid * (1.0 + gate_all * (1.0 - gate_sigmoid))
    grad_up = grad_h * gate_silu
    grad_hidden = jnp.concatenate([grad_gate.astype(BF), grad_up.astype(BF)], axis=1)

    blocks = grad_hidden.reshape(2, ny, tokens // ny, 2 * width)
    own_cols, other_cols = {}, {}
    for pair in ((0, 1), (3, 2)):
        w = jnp.concatenate([gates[q] for q in pair])
        total = None
        for j in (1, 2, 3, 0):
            rows = lax.dynamic_index_in_dim(blocks, (yi + j) % ny, 1, keepdims=False)
            part = lax.dot_general(
                rows.reshape(-1, 2 * width),
                w,
                (((1,), (1,)), ((), ())),
                preferred_element_type=F32,
            )
            if j:
                part = shift(part.astype(BF), Y, j).astype(F32)
            total = part if total is None else total + part
        cols = total.shape[1]
        total = total.astype(BF).reshape(2, nz, -1, cols)
        summed = None
        for j in (1, 2, 3, 0):
            part = lax.dynamic_index_in_dim(total, (zh + j) % nz, 1, keepdims=False)
            if j:
                part = shift(part, ZH, j)
            part = part.astype(F32)
            summed = part if summed is None else summed + part
        summed = summed.astype(BF)
        got = shift(summed[1], C, 1)
        for i, q in enumerate(pair):
            own_cols[q] = summed[0][:, i * 2 * slab : (i + 1) * 2 * slab]
            other_cols[q] = got[:, i * 2 * slab : (i + 1) * 2 * slab]
    piece = from_slabs(
        [own_cols[q] for q in range(nx)], [other_cols[q] for q in range(nx)], pos_back, slab
    )
    by_z = [piece] + [shift(piece, ZH, j) for j in (1, 2, 3)]
    rows = piece.shape[0]
    grad_input = jnp.zeros((ny, nz, rows, piece.shape[1]), BF)
    rest = jnp.stack(by_z[1:])
    for j in range(ny):
        first = shift(piece, Y, j) if j else piece
        others = shift(rest, Y, j) if j else rest
        at = (yi - j) % ny
        grad_input = lax.dynamic_update_slice(
            grad_input, first[None, None], (at, zh, 0, 0)
        )
        for k in (1, 2, 3):
            grad_input = lax.dynamic_update_slice(
                grad_input, others[None, k - 1 : k], (at, (zh - k) % nz, 0, 0)
            )
    grad_input = grad_input.reshape(tokens, -1)

    def down_block(q):
        return lax.dot_general(
            out_all[q], hidden, (((0,), (0,)), ((), ())), preferred_element_type=F32
        )

    def gate_block(q):
        return lax.dot_general(
            act_all[q], grad_hidden, (((0,), (0,)), ((), ())), preferred_element_type=F32
        )

    grad_down = scatter_pairs(down_block) / dp_count
    grad_gate_up = (scatter_pairs(gate_block) / dp_count).reshape(slab, 2, width)
    return (grad_input, grad_gate_up, grad_down)


def solution(mesh):
    split = Mesh(
        mesh.devices.reshape(2, 4, 2, 4, 4), ("dp_0", "dp_1", "dp_2", "tensor_0", "tensor_1")
    )
    return jax.shard_map(
        per_device,
        mesh=split,
        in_specs=(
            P(DP, None),
            P(DP, None),
            P(DP, TENSOR),
            P(DP, TENSOR),
            P(DP, None, TENSOR),
            P(DP, TENSOR),
        ),
        out_specs=(P(DP, None), P(DP, None, TENSOR), P(DP, TENSOR)),
        check_vma=False,
    )
```

```python
import functools

import jax
import jax.numpy as jnp
from jax import lax
from jax.experimental import pallas as pl
from jax.experimental.pallas import tpu as pltpu
from jax.sharding import Mesh
from jax.sharding import PartitionSpec as P

Z, X, C = "dp_0", "dp_1", "dp_2"
DP = (Z, X, C)
ZH, Y = "tensor_0", "tensor_1"
TENSOR = (ZH, Y)
BF = jnp.bfloat16
F32 = jnp.float32


def ring(v):
    n = lax.axis_size(X)
    pairs = []
    for i in range(n):
        pairs.append((2 * i, 2 * ((i + 1) % n)))
        pairs.append((2 * i + 1, 2 * ((i - 1) % n) + 1))
    return lax.ppermute(v, (X, C), pairs)


def swap(v, axis):
    return lax.ppermute(v, axis, [(0, 1), (1, 0)])


def to_slabs_kernel(pos_ref, x_ref, mine_ref, theirs_ref, *, slab, nx):
    for z in range(2):
        for core in range(2):

            @pl.when((pos_ref[0] == z) & (pos_ref[1] == core))
            def _(z=z, core=core):
                for xx in range(nx):
                    q = pos_ref[2 + xx]
                    back = (nx - q) % nx
                    for zz in range(2):
                        k = zz * nx + xx
                        half = slice((zz ^ z) * slab, ((zz ^ z) + 1) * slab)
                        m = 2 * k + core
                        t = 2 * k + 1 - core
                        mine_ref[q, :, half] = x_ref[:, m * slab : (m + 1) * slab]
                        theirs_ref[back, :, half] = x_ref[:, t * slab : (t + 1) * slab]


def to_slabs(x, pos, slab, nx):
    tokens, width = x.shape
    rows = 64
    out = jax.ShapeDtypeStruct((nx, tokens, 2 * slab), x.dtype)
    return pl.pallas_call(
        functools.partial(to_slabs_kernel, slab=slab, nx=nx),
        grid_spec=pltpu.PrefetchScalarGridSpec(
            num_scalar_prefetch=1,
            grid=(tokens // rows,),
            in_specs=[pl.BlockSpec((rows, width), lambda i, s: (i, 0))],
            out_specs=[pl.BlockSpec((nx, rows, 2 * slab), lambda i, s: (0, i, 0))] * 2,
        ),
        out_shape=[out, out],
        name="to_slabs",
    )(pos, x)


def from_slabs_kernel(pos_ref, *refs, slab, nx):
    own_refs, other_refs, o_ref = refs[:nx], refs[nx : 2 * nx], refs[-1]
    z_odd = pos_ref[0] == 1
    core_odd = pos_ref[1] == 1
    shift_by = pos_ref[2]

    def placed(rs, backward):
        v = [r[...] for r in rs]
        v = [jnp.where(backward, v[(nx - i) % nx], v[i]) for i in range(nx)]
        for s in (1, 2):
            on = (shift_by & s) != 0
            v = [jnp.where(on, v[(i - s) % nx], v[i]) for i in range(nx)]
        return v

    own = placed(own_refs, jnp.logical_not(core_odd))
    other = placed(other_refs, core_odd)
    for xx in range(nx):
        halves = []
        for v in (own, other):
            near, far = v[xx][:, :slab], v[xx][:, slab:]
            halves.append((jnp.where(z_odd, far, near), jnp.where(z_odd, near, far)))
        for zz in range(2):
            k = zz * nx + xx
            mine, theirs = halves[0][zz], halves[1][zz]
            even = jnp.where(core_odd, theirs, mine)
            odd = jnp.where(core_odd, mine, theirs)
            both = jnp.concatenate([even, odd], axis=1)
            for i in range(o_ref.shape[0]):
                o_ref[i, :, 2 * k * slab : (2 * k + 2) * slab] = both


def from_slabs(own, other, pos, slab, copies):
    nx = len(own)
    rows = own[0].shape[0]
    return pl.pallas_call(
        functools.partial(from_slabs_kernel, slab=slab, nx=nx),
        in_specs=[pl.BlockSpec(memory_space=pltpu.SMEM)]
        + [pl.BlockSpec(memory_space=pltpu.VMEM)] * (2 * nx),
        out_shape=jax.ShapeDtypeStruct((copies, rows, 4 * nx * slab), own[0].dtype),
        name="from_slabs",
    )(pos, *own, *other)


def interleave(own, other, rows):
    *lead, tokens, width = own.shape
    cut = (*lead, tokens // rows, 1, rows, width)
    both = jnp.concatenate([own.reshape(cut), other.reshape(cut)], axis=len(lead) + 1)
    return both.reshape(*lead, 2 * tokens, width)


def per_device(activations, grad_out, gate_pre, up_pre, gate_up, down_weight):
    tokens = activations.shape[0]
    slab, width = down_weight.shape
    nx, ny, nz = lax.axis_size(X), lax.axis_size(Y), lax.axis_size(ZH)
    dp_count = lax.axis_size(DP)
    rows = tokens // (ny * nz)
    xi, zi, ci = lax.axis_index(X), lax.axis_index(Z), lax.axis_index(C)
    sign = 2 * ci - 1
    pos = jnp.stack([zi, ci] + [(sign * (k - xi)) & (nx - 1) for k in range(nx)]).astype(jnp.int32)
    pos_back = jnp.stack([zi, ci, xi]).astype(jnp.int32)

    down_near, gate_near = [down_weight], [gate_up.reshape(slab, 2 * width)]
    down_far = [swap(down_near[0], Z)]
    for _ in range(nx - 1):
        down_near.append(ring(down_near[-1]))
        down_far.append(ring(down_far[-1]))
    gates = [jnp.concatenate([gate_near[0], swap(gate_near[0], Z)])]
    for _ in range(nx - 1):
        gates.append(ring(gates[-1]))
    down = [jnp.concatenate([a, b]) for a, b in zip(down_near, down_far)]

    out_mine, out_theirs = to_slabs(grad_out, pos, slab, nx)
    out_all = interleave(out_mine, swap(out_theirs, C), rows)
    gate_all = interleave(gate_pre, swap(gate_pre, C), rows).astype(F32)
    up_all = interleave(up_pre, swap(up_pre, C), rows).astype(F32)
    act_mine, act_theirs = to_slabs(activations, pos, slab, nx)
    act_all = interleave(act_mine, swap(act_theirs, C), rows)

    gate_sigmoid = jax.nn.sigmoid(gate_all)
    gate_silu = gate_all * gate_sigmoid
    hidden = (gate_silu * up_all).astype(BF)

    part_h = sum(jnp.dot(out_all[q], down[q], preferred_element_type=F32) for q in range(nx))
    got_h = swap(part_h, C).reshape(ny * nz, 2, rows, width)
    got_h = jnp.concatenate([got_h[:, 1:], got_h[:, :1]], axis=1).reshape(part_h.shape)
    grad_h = part_h + got_h
    grad_gate = grad_h * up_all * gate_sigmoid * (1.0 + gate_all * (1.0 - gate_sigmoid))
    grad_up = grad_h * gate_silu
    grad_hidden = jnp.concatenate([grad_gate.astype(BF), grad_up.astype(BF)], axis=1)

    own_cols, other_cols = [], []
    for pair in ((0, 1), (2, 3)):
        w = jnp.concatenate([gates[q] for q in pair])
        part = lax.dot_general(
            grad_hidden, w, (((1,), (1,)), ((), ())), preferred_element_type=F32
        ).astype(BF)
        for axis in (Y, ZH):
            n = lax.axis_size(axis)
            part = lax.all_to_all(part.reshape(n, -1, part.shape[-1]), axis, 0, 0, tiled=True)
            part = jnp.sum(part.astype(F32), axis=0).astype(BF)
        got = swap(part[rows:], C)
        for i in range(2):
            own_cols.append(part[:rows, i * 2 * slab : (i + 1) * 2 * slab])
            other_cols.append(got[:, i * 2 * slab : (i + 1) * 2 * slab])
    piece = from_slabs(own_cols, other_cols, pos_back, slab, nz)
    piece = lax.all_to_all(piece, ZH, 0, 0, tiled=True)
    piece = piece.reshape(1, nz * rows, -1)
    grad_input = lax.all_to_all(
        jnp.broadcast_to(piece, (ny, *piece.shape[1:])), Y, 0, 0, tiled=True
    ).reshape(tokens, -1)

    down_blocks = [
        lax.dot_general(out_all[q], hidden, (((0,), (0,)), ((), ())), preferred_element_type=F32)
        for q in range(nx)
    ]
    got = swap(jnp.stack([b[slab:].astype(BF) for b in down_blocks]), Z)
    down_sums = [b[:slab] + got[q].astype(F32) for q, b in enumerate(down_blocks)]
    grad_down = down_sums[1]
    for q in (2, 3, 0):
        grad_down = down_sums[q] + ring(grad_down.astype(BF)).astype(F32)

    def gate_block(q):
        return lax.dot_general(
            act_all[q], grad_hidden, (((0,), (0,)), ((), ())), preferred_element_type=F32
        )

    total = gate_block(1)
    for q in (2, 3, 0):
        total = gate_block(q) + ring(total.astype(BF)).astype(F32)
    grad_gate_up = total[:slab] + swap(total[slab:].astype(BF), Z).astype(F32)
    grad_gate_up = (grad_gate_up / dp_count).reshape(slab, 2, width)
    return (grad_input, grad_gate_up, grad_down / dp_count)


def solution(mesh):
    split = Mesh(
        mesh.devices.reshape(2, 4, 2, 4, 4), ("dp_0", "dp_1", "dp_2", "tensor_0", "tensor_1")
    )
    return jax.shard_map(
        per_device,
        mesh=split,
        in_specs=(
            P(DP, None),
            P(DP, None),
            P(DP, TENSOR),
            P(DP, TENSOR),
            P(DP, None, TENSOR),
            P(DP, TENSOR),
        ),
        out_specs=(P(DP, None), P(DP, None, TENSOR), P(DP, TENSOR)),
        check_vma=False,
    )
```

```python
import functools

import jax
import jax.numpy as jnp
from jax import lax
from jax.experimental import pallas as pl
from jax.experimental.pallas import tpu as pltpu
from jax.sharding import Mesh
from jax.sharding import PartitionSpec as P

Z, X, C = "dp_0", "dp_1", "dp_2"
DP = (Z, X, C)
ZH, Y = "tensor_0", "tensor_1"
TENSOR = (ZH, Y)
BF = jnp.bfloat16
F32 = jnp.float32


def shift(v, axis, step):
    n = lax.axis_size(axis)
    return lax.ppermute(v, axis, [(i, (i + step) % n) for i in range(n)])


def ring(v):
    n = lax.axis_size(X)
    pairs = []
    for i in range(n):
        pairs.append((2 * i, 2 * ((i + 1) % n)))
        pairs.append((2 * i + 1, 2 * ((i - 1) % n) + 1))
    return lax.ppermute(v, (X, C), pairs)


def swap(v, axis):
    return lax.ppermute(v, axis, [(0, 1), (1, 0)])


def to_slabs_kernel(pos_ref, x_ref, mine_ref, theirs_ref, *, slab, nx, by_chip):
    z = pos_ref[0]
    for core in range(2):
        for odd in range(2):

            @pl.when((pos_ref[1] == core) & (pos_ref[2] == odd))
            def _(core=core, odd=odd):
                for xx in range(nx):
                    q = pos_ref[3 + xx]
                    for ref, side, hops in (
                        (mine_ref, core, q),
                        (theirs_ref, 1 - core, (nx - q) & (nx - 1)),
                    ):
                        for zz in range(2):
                            far = zz ^ z
                            k = 2 * (zz * nx + xx) + side
                            v = x_ref[:, k * slab : (k + 1) * slab]
                            if by_chip:
                                for d in range(2):

                                    @pl.when(far == d)
                                    def _(v=v, d=d, ref=ref, hops=hops):
                                        ref[hops, :, d * slab : (d + 1) * slab] = v

                            else:
                                d = (xx + odd) % 2
                                ref[far * (nx // 2) + hops // 2, :, d * slab : (d + 1) * slab] = v


def to_slabs(x, pos, slab, nx, by_chip):
    tokens, width = x.shape
    rows = 64
    out = jax.ShapeDtypeStruct((nx, tokens, 2 * slab), x.dtype)
    return pl.pallas_call(
        functools.partial(to_slabs_kernel, slab=slab, nx=nx, by_chip=by_chip),
        grid_spec=pltpu.PrefetchScalarGridSpec(
            num_scalar_prefetch=1,
            grid=(tokens // rows,),
            in_specs=[pl.BlockSpec((rows, width), lambda i, s: (i, 0))],
            out_specs=[pl.BlockSpec((nx, rows, 2 * slab), lambda i, s: (0, i, 0))] * 2,
        ),
        out_shape=[out, out],
        name="to_slabs",
    )(pos, x)


def factors_kernel(g0_ref, g1_ref, u0_ref, u1_ref, hidden_ref, gate_ref, up_ref):
    tokens = g0_ref.shape[1]
    for a, (g_ref, u_ref) in enumerate(((g0_ref, u0_ref), (g1_ref, u1_ref))):
        at = slice(a * tokens, (a + 1) * tokens)
        g = g_ref[...].astype(F32)
        u = u_ref[...].astype(F32)
        s = 1.0 / (1.0 + jnp.exp(-g))
        silu = g * s
        hidden_ref[:, at] = (silu * u).astype(BF)
        gate_ref[:, at] = u * s * (1.0 + g * (1.0 - s))
        up_ref[:, at] = silu


def factors(*args):
    width, tokens = args[0].shape
    outs = [jax.ShapeDtypeStruct((width, 2 * tokens), t) for t in (BF, F32, F32)]
    return pl.pallas_call(factors_kernel, out_shape=outs, name="factors")(*args)


def grad_hidden_kernel(part_ref, got_ref, gate_ref, up_ref, o_ref):
    width, both = part_ref.shape
    tokens = both // 2
    for a in range(2):
        at = slice(a * tokens, (a + 1) * tokens)
        h = part_ref[:, at] + got_ref[:, tokens - a * tokens : both - a * tokens]
        o_ref[:width, at] = (h * gate_ref[:, at]).astype(BF)
        o_ref[width:, at] = (h * up_ref[:, at]).astype(BF)


def grad_hidden_of(part, got, gate, up):
    width, both = part.shape
    return pl.pallas_call(
        grad_hidden_kernel,
        out_shape=jax.ShapeDtypeStruct((2 * width, both), BF),
        name="grad_hidden",
    )(part, got, gate, up)


def from_slabs_kernel(pos_ref, own_ref, other_ref, o_ref, *, slab, mixed):
    z_odd = pos_ref[0] == 1
    core_odd = pos_ref[1] == 1

    def halves(ref, swapped):
        v = ref[...]
        pair = [v[:, : 2 * slab], v[:, 2 * slab :]]
        if mixed:
            pair = [jnp.where(swapped, pair[1 - i], pair[i]) for i in range(2)]
        out = []
        for p in pair:
            near, far = p[:, :slab], p[:, slab:]
            out.append((jnp.where(z_odd, far, near), jnp.where(z_odd, near, far)))
        return out

    own = halves(own_ref, core_odd)
    other = halves(other_ref, jnp.logical_not(core_odd))
    for i in range(2):
        for zz in range(2):
            even = jnp.where(core_odd, other[i][zz], own[i][zz])
            odd = jnp.where(core_odd, own[i][zz], other[i][zz])
            both = jnp.concatenate([even, odd], axis=1)
            at = (2 * i + zz) * 2 * slab
            o_ref[:, at : at + 2 * slab] = both


def from_slabs(own, other, pos, slab, mixed):
    rows, cols = own.shape
    vmem = pl.BlockSpec(memory_space=pltpu.VMEM)
    return pl.pallas_call(
        functools.partial(from_slabs_kernel, slab=slab, mixed=mixed),
        in_specs=[pl.BlockSpec(memory_space=pltpu.SMEM), vmem, vmem],
        out_shape=jax.ShapeDtypeStruct((rows, 2 * cols), own.dtype),
        name="from_slabs",
    )(pos, own, other)


def assemble_kernel(pos_ref, a_ref, b_ref, o_ref, sems, *, block, nx):
    xi = pos_ref[2]
    copies = []
    for n, (ref, dxs) in enumerate(((a_ref, (0, 2)), (b_ref, (nx - 1, 1)))):
        for i, dx in enumerate(dxs):
            x = (xi + dx) & (nx - 1)
            for zz in range(2):
                src = (2 * i + zz) * block
                dst = pl.multiple_of((zz * nx + x) * block, 128)
                copies.append(
                    pltpu.make_async_copy(
                        ref.at[:, src : src + block],
                        o_ref.at[:, pl.ds(dst, block)],
                        sems.at[n * 4 + i * 2 + zz],
                    )
                )
    for c in copies:
        c.start()
    for c in copies:
        c.wait()


def assemble(a, b, pos, block, nx):
    rows, cols = a.shape
    hbm = pl.BlockSpec(memory_space=pl.ANY)
    return pl.pallas_call(
        functools.partial(assemble_kernel, block=block, nx=nx),
        in_specs=[pl.BlockSpec(memory_space=pltpu.SMEM), hbm, hbm],
        out_specs=hbm,
        out_shape=jax.ShapeDtypeStruct((rows, 2 * cols), a.dtype),
        scratch_shapes=[pltpu.SemaphoreType.DMA((8,))],
        name="assemble",
    )(pos, a, b)


def sum_blocks_kernel(pos_ref, x_ref, *o_refs):
    n = len(o_refs)
    for j, o_ref in enumerate(o_refs):
        at = (pos_ref[3] + j) & (n - 1)
        total = x_ref[0, at].astype(F32)
        for i in range(1, x_ref.shape[0]):
            total = total + x_ref[i, at].astype(F32)
        o_ref[...] = total.astype(BF)


def sum_blocks(x, pos, n):
    m, rows, cols = x.shape
    out = jax.ShapeDtypeStruct((rows // n, cols), BF)
    return pl.pallas_call(
        sum_blocks_kernel,
        in_specs=[
            pl.BlockSpec(memory_space=pltpu.SMEM),
            pl.BlockSpec(memory_space=pltpu.VMEM),
        ],
        out_shape=[out] * n,
        name="sum_blocks",
    )(pos, x.reshape(m, n, rows // n, cols))


def spread_kernel(pos_ref, *refs):
    o_ref = refs[-1]
    n = len(refs) - 1
    for j, ref in enumerate(refs[:-1]):
        v = ref[...]
        for i in range(o_ref.shape[0]):
            o_ref[i, (pos_ref[3] - j) & (n - 1)] = v


def spread(pieces, pos, copies):
    n = len(pieces)
    rows, cols = pieces[0].shape
    out = pl.pallas_call(
        spread_kernel,
        in_specs=[pl.BlockSpec(memory_space=pltpu.SMEM)]
        + [pl.BlockSpec(memory_space=pltpu.VMEM)] * n,
        out_shape=jax.ShapeDtypeStruct((copies, n, rows, cols), BF),
        name="spread",
    )(pos, *pieces)
    return out.reshape(copies, n * rows, cols)


def layer(activations, grad_out, gate_pre, up_pre, gate_up, down_weight):
    tokens = activations.shape[0]
    slab, width = down_weight.shape
    nx, ny, nz = lax.axis_size(X), lax.axis_size(Y), lax.axis_size(ZH)
    dp_count = lax.axis_size(DP)
    rows = tokens // (ny * nz)
    xi, zi, ci = lax.axis_index(X), lax.axis_index(Z), lax.axis_index(C)
    zh = lax.axis_index(ZH)
    sign = 2 * ci - 1
    pos = jnp.stack(
        [zi, ci, xi & 1] + [(sign * (k - xi)) & (nx - 1) for k in range(nx)]
    ).astype(jnp.int32)
    pos_back = jnp.stack([zi, ci, xi, zh]).astype(jnp.int32)

    near, far = [down_weight], []
    far.append(swap(down_weight, Z))
    for _ in range(1, nx):
        near.append(ring(near[-1]))
        far.append(ring(far[-1]))
    gate_near = gate_up.reshape(slab, 2 * width)
    gates = [jnp.concatenate([gate_near, swap(gate_near, Z)])]
    for _ in range(1, nx):
        gates.append(ring(gates[-1]))

    out_mine, out_theirs = to_slabs(grad_out, pos, slab, nx, False)
    out_theirs = swap(out_theirs, C)
    out_all = jnp.concatenate([out_mine, out_theirs], axis=1)
    gate_other = swap(gate_pre.T, C)
    up_other = swap(up_pre.T, C)
    hidden, gate_factor, up_factor = factors(gate_pre.T, gate_other, up_pre.T, up_other)
    act_mine, act_theirs = to_slabs(activations, pos, slab, nx, True)
    act_theirs = swap(act_theirs, C)
    act_all = jnp.concatenate([act_mine, act_theirs], axis=1)

    part_h = None
    for k, pieces in ((0, near[:2]), (2, far[:2]), (1, near[2:]), (3, far[2:])):
        p = lax.dot_general(
            jnp.concatenate(pieces),
            out_all[k],
            (((0,), (1,)), ((), ())),
            preferred_element_type=F32,
        )
        part_h = p if part_h is None else part_h + p
    got_h = swap(part_h, C)
    grad_hidden = grad_hidden_of(part_h, got_h, gate_factor, up_factor)

    def down_block(k):
        return lax.dot_general(
            out_all[k], hidden, (((0,), (1,)), ((), ())), preferred_element_type=F32
        )

    sums = []
    for k in (0, 1):
        got = swap(down_block(2 + k).astype(BF), Z)
        both = down_block(k) + got.astype(F32)
        sums += [both[:slab], both[slab:]]
    grad_down = sums[1]
    for q in (2, 3, 0):
        grad_down = sums[q] + ring(grad_down.astype(BF)).astype(F32)

    chunks = []
    for n, pair in enumerate(((0, 2), (1, 3))):
        w = jnp.concatenate([gates[q] for q in pair])
        part = lax.dot_general(
            grad_hidden, w, (((0,), (1,)), ((), ())), preferred_element_type=F32
        ).astype(BF)
        part = part.reshape(2, ny * nz, rows, part.shape[1]).transpose(1, 0, 2, 3)
        part = lax.all_to_all(part.reshape(ny, -1, part.shape[-1]), Y, 0, 0, tiled=True)
        blocks = sum_blocks(part, pos_back, nz)
        part = blocks[0].astype(F32)
        for j in range(1, nz):
            got = shift(blocks[j], ZH, j)
            part = part + got.astype(F32)
        part = part.astype(BF)
        got = swap(part[rows:], C)
        piece = from_slabs(part[:rows], got, pos_back, slab, n == 1)
        pieces = [piece]
        for j in range(1, nz):
            pieces.append(shift(piece, ZH, j))
        piece = spread(pieces, pos_back, ny)
        piece = lax.all_to_all(piece, Y, 0, 0, tiled=True)
        chunks.append(piece.reshape(tokens, -1))
    grad_input = assemble(*chunks, pos_back, 2 * slab, nx)

    def gate_block(q):
        return lax.dot_general(
            act_all[q], grad_hidden, (((0,), (1,)), ((), ())), preferred_element_type=F32
        )

    total = gate_block(1)
    for q in (2, 3, 0):
        total = gate_block(q) + ring(total.astype(BF)).astype(F32)
    grad_gate_up = total[:slab] + swap(total[slab:].astype(BF), Z).astype(F32)
    grad_gate_up = (grad_gate_up / dp_count).reshape(slab, 2, width)
    return (grad_input, grad_gate_up, grad_down / dp_count)


def solution(mesh):
    split = Mesh(
        mesh.devices.reshape(2, 4, 2, 4, 4), ("dp_0", "dp_1", "dp_2", "tensor_0", "tensor_1")
    )
    return jax.shard_map(
        layer,
        mesh=split,
        in_specs=(
            P(DP, None),
            P(DP, None),
            P(DP, TENSOR),
            P(DP, TENSOR),
            P(DP, None, TENSOR),
            P(DP, TENSOR),
        ),
        out_specs=(P(DP, None), P(DP, None, TENSOR), P(DP, TENSOR)),
        check_vma=False,
    )
```

```python
import functools

import jax
import jax.numpy as jnp
from jax import lax
from jax.experimental import pallas as pl
from jax.experimental.pallas import tpu as pltpu
from jax.sharding import Mesh
from jax.sharding import PartitionSpec as P

Z, X, C = "dp_0", "dp_1", "dp_2"
DP = (Z, X, C)
ZH, Y = "tensor_0", "tensor_1"
TENSOR = (ZH, Y)
BF = jnp.bfloat16
F32 = jnp.float32


def shift(v, axis, step):
    n = lax.axis_size(axis)
    return lax.ppermute(v, axis, [(i, (i + step) % n) for i in range(n)])


def ring(v):
    n = lax.axis_size(X)
    pairs = []
    for i in range(n):
        pairs.append((2 * i, 2 * ((i + 1) % n)))
        pairs.append((2 * i + 1, 2 * ((i - 1) % n) + 1))
    return lax.ppermute(v, (X, C), pairs)


def swap(v, axis):
    return lax.ppermute(v, axis, [(0, 1), (1, 0)])


def to_slabs_kernel(pos_ref, x_ref, mine_ref, theirs_ref, *, slab, nx):
    z = pos_ref[0]
    for core in range(2):
        for odd in range(2):

            @pl.when((pos_ref[1] == core) & (pos_ref[2] == odd))
            def _(core=core, odd=odd):
                for xx in range(nx):
                    q = pos_ref[3 + xx]
                    for ref, side, hops in (
                        (mine_ref, core, q),
                        (theirs_ref, 1 - core, (nx - q) & (nx - 1)),
                    ):
                        for zz in range(2):
                            far = zz ^ z
                            k = 2 * (zz * nx + xx) + side
                            v = x_ref[:, k * slab : (k + 1) * slab]
                            d = (xx + odd) % 2
                            ref[far * (nx // 2) + hops // 2, :, d * slab : (d + 1) * slab] = v


def to_slabs(x, pos, slab, nx):
    tokens, width = x.shape
    rows = 64
    out = jax.ShapeDtypeStruct((nx, tokens, 2 * slab), x.dtype)
    return pl.pallas_call(
        functools.partial(to_slabs_kernel, slab=slab, nx=nx),
        grid_spec=pltpu.PrefetchScalarGridSpec(
            num_scalar_prefetch=1,
            grid=(tokens // rows,),
            in_specs=[pl.BlockSpec((rows, width), lambda i, s: (i, 0))],
            out_specs=[pl.BlockSpec((nx, rows, 2 * slab), lambda i, s: (0, i, 0))] * 2,
        ),
        out_shape=[out, out],
        name="to_slabs",
    )(pos, x)


def to_columns_kernel(pos_ref, x_ref, mine_ref, theirs_ref, *, slab):
    for core in range(2):

        @pl.when(pos_ref[1] == core)
        def _(core=core):
            for k in range(x_ref.shape[1] // (2 * slab)):
                for ref, side in ((mine_ref, core), (theirs_ref, 1 - core)):
                    at = (2 * k + side) * slab
                    ref[:, k * slab : (k + 1) * slab] = x_ref[:, at : at + slab]


def to_columns(x, pos, slab):
    tokens, width = x.shape
    rows = 64
    out = jax.ShapeDtypeStruct((tokens, width // 2), x.dtype)
    return pl.pallas_call(
        functools.partial(to_columns_kernel, slab=slab),
        grid_spec=pltpu.PrefetchScalarGridSpec(
            num_scalar_prefetch=1,
            grid=(tokens // rows,),
            in_specs=[pl.BlockSpec((rows, width), lambda i, s: (i, 0))],
            out_specs=[pl.BlockSpec((rows, width // 2), lambda i, s: (i, 0))] * 2,
        ),
        out_shape=[out, out],
        name="to_columns",
    )(pos, x)


def factors_kernel(g0_ref, g1_ref, u0_ref, u1_ref, hidden_ref, gate_ref, up_ref):
    tokens = g0_ref.shape[1]
    for a, (g_ref, u_ref) in enumerate(((g0_ref, u0_ref), (g1_ref, u1_ref))):
        at = slice(a * tokens, (a + 1) * tokens)
        g = g_ref[...].astype(F32)
        u = u_ref[...].astype(F32)
        s = 1.0 / (1.0 + jnp.exp(-g))
        silu = g * s
        hidden_ref[:, at] = (silu * u).astype(BF)
        gate_ref[:, at] = u * s * (1.0 + g * (1.0 - s))
        up_ref[:, at] = silu


def factors(*args):
    width, tokens = args[0].shape
    outs = [jax.ShapeDtypeStruct((width, 2 * tokens), t) for t in (BF, F32, F32)]
    return pl.pallas_call(factors_kernel, out_shape=outs, name="factors")(*args)


def grad_hidden_kernel(part_ref, got_ref, gate_ref, up_ref, o_ref):
    width, both = part_ref.shape
    tokens = both // 2
    for a in range(2):
        at = slice(a * tokens, (a + 1) * tokens)
        h = part_ref[:, at] + got_ref[:, tokens - a * tokens : both - a * tokens]
        o_ref[:width, at] = (h * gate_ref[:, at]).astype(BF)
        o_ref[width:, at] = (h * up_ref[:, at]).astype(BF)


def grad_hidden_of(part, got, gate, up):
    width, both = part.shape
    return pl.pallas_call(
        grad_hidden_kernel,
        out_shape=jax.ShapeDtypeStruct((2 * width, both), BF),
        name="grad_hidden",
    )(part, got, gate, up)


def cut_kernel(pos_ref, x_ref, *o_refs):
    n = len(o_refs)
    for j, o_ref in enumerate(o_refs):
        at = (pos_ref[3] + j) & (n - 1)
        for a in range(2):
            o_ref[:, a] = x_ref[a, at]


def cut(x, pos, n, m, rows):
    cols = x.shape[1]
    out = jax.ShapeDtypeStruct((m, 2, rows, cols), x.dtype)
    outs = pl.pallas_call(
        cut_kernel,
        in_specs=[
            pl.BlockSpec(memory_space=pltpu.SMEM),
            pl.BlockSpec(memory_space=pltpu.VMEM),
        ],
        out_shape=[out] * n,
        name="cut",
    )(pos, x.reshape(2, n, m, rows, cols))
    return [o.reshape(m * 2 * rows, cols) for o in outs]


def from_slabs_kernel(pos_ref, own_ref, other_ref, o_ref, *, slab):
    core_odd = pos_ref[1] == 1
    own, other = own_ref[...], other_ref[...]
    for i in range(own.shape[1] // slab):
        mine, theirs = (v[:, i * slab : (i + 1) * slab] for v in (own, other))
        even = jnp.where(core_odd, theirs, mine)
        odd = jnp.where(core_odd, mine, theirs)
        both = jnp.concatenate([even, odd], axis=1)
        for n in range(o_ref.shape[0]):
            o_ref[n, :, 2 * i * slab : 2 * (i + 1) * slab] = both


def from_slabs(own, other, pos, slab, copies):
    rows, cols = own.shape
    vmem = pl.BlockSpec(memory_space=pltpu.VMEM)
    return pl.pallas_call(
        functools.partial(from_slabs_kernel, slab=slab),
        in_specs=[pl.BlockSpec(memory_space=pltpu.SMEM), vmem, vmem],
        out_shape=jax.ShapeDtypeStruct((copies, rows, 2 * cols), own.dtype),
        name="from_slabs",
    )(pos, own, other)


def assemble_kernel(pos_ref, *refs, block, nx, ny):
    o_ref = refs[-1]
    zi, xi, yi = pos_ref[0], pos_ref[2], pos_ref[3]
    rows = refs[0].shape[0]
    for n in range(nx // 2):
        for j in range(ny):
            ref = refs[n * ny + j]
            row = pl.multiple_of(((yi - j) & (ny - 1)) * rows, rows)
            for i in range(2):
                q = 2 * n + i
                for d, at in enumerate((zi * nx + ((xi - q) & (nx - 1)), (1 - zi) * nx + ((xi + q) & (nx - 1)))):
                    src = (2 * i + d) * block
                    o_ref[pl.ds(row, rows), pl.ds(pl.multiple_of(at * block, 128), block)] = ref[
                        :, src : src + block
                    ]


def assemble(pieces, pos, block, nx, ny):
    rows, cols = pieces[0].shape
    vmem = pl.BlockSpec(memory_space=pltpu.VMEM)
    return pl.pallas_call(
        functools.partial(assemble_kernel, block=block, nx=nx, ny=ny),
        in_specs=[pl.BlockSpec(memory_space=pltpu.SMEM)] + [vmem] * len(pieces),
        out_shape=jax.ShapeDtypeStruct((ny * rows, (nx // 2) * cols), pieces[0].dtype),
        name="assemble",
    )(pos, *pieces)


def layer(activations, grad_out, gate_pre, up_pre, gate_up, down_weight):
    tokens = activations.shape[0]
    slab, width = down_weight.shape
    nx, ny, nz = lax.axis_size(X), lax.axis_size(Y), lax.axis_size(ZH)
    dp_count = lax.axis_size(DP)
    rows = tokens // (ny * nz)
    xi, zi, ci = lax.axis_index(X), lax.axis_index(Z), lax.axis_index(C)
    yi = lax.axis_index(Y)
    sign = 2 * ci - 1
    pos = jnp.stack(
        [zi, ci, xi & 1] + [(sign * (k - xi)) & (nx - 1) for k in range(nx)]
    ).astype(jnp.int32)
    pos_back = jnp.stack([zi, ci, xi, yi]).astype(jnp.int32)

    near, far = [down_weight], []
    far.append(swap(down_weight, Z))
    for _ in range(1, nx):
        near.append(ring(near[-1]))
        far.append(ring(far[-1]))
    gate_near = gate_up.reshape(slab, 2 * width)
    gate_far = [swap(gate_near, Z)]
    gate_near = [gate_near]
    for _ in range(1, nx):
        gate_near.append(shift(gate_near[-1], X, 1))
        gate_far.append(shift(gate_far[-1], X, -1))

    out_mine, out_theirs = to_slabs(grad_out, pos, slab, nx)
    out_theirs = swap(out_theirs, C)
    out_all = jnp.concatenate([out_mine, out_theirs], axis=1)
    gate_other = swap(gate_pre.T, C)
    up_other = swap(up_pre.T, C)
    hidden, gate_factor, up_factor = factors(gate_pre.T, gate_other, up_pre.T, up_other)
    act_mine, act_theirs = to_columns(activations, pos, slab)
    act_theirs = swap(act_theirs, C)
    act_all = jnp.concatenate([act_mine, act_theirs])

    part_h = None
    for k, pieces in ((0, near[:2]), (2, far[:2]), (1, near[2:]), (3, far[2:])):
        p = lax.dot_general(
            jnp.concatenate(pieces),
            out_all[k],
            (((0,), (1,)), ((), ())),
            preferred_element_type=F32,
        )
        part_h = p if part_h is None else part_h + p
    got_h = swap(part_h, C)
    grad_hidden = grad_hidden_of(part_h, got_h, gate_factor, up_factor)

    def down_block(k):
        return lax.dot_general(
            out_all[k], hidden, (((0,), (1,)), ((), ())), preferred_element_type=F32
        )

    sums = []
    for k in (0, 1):
        got = swap(down_block(2 + k).astype(BF), Z)
        both = down_block(k) + got.astype(F32)
        sums += [both[:slab], both[slab:]]
    grad_down = sums[1]
    for q in (2, 3, 0):
        grad_down = sums[q] + ring(grad_down.astype(BF)).astype(F32)

    pieces = []
    for n in range(2):
        w = jnp.concatenate(
            [g[q] for q in (2 * n, 2 * n + 1) for g in (gate_near, gate_far)]
        )
        part = lax.dot_general(
            grad_hidden, w, (((0,), (1,)), ((), ())), preferred_element_type=F32
        ).astype(BF)
        blocks = cut(part, pos_back, ny, nz, rows)
        part = blocks[0].astype(F32)
        for j in range(1, ny):
            got = shift(blocks[j], Y, j)
            part = part + got.astype(F32)
        part = part.astype(BF).reshape(nz, 2 * rows, -1)
        part = lax.all_to_all(part, ZH, 0, 0, tiled=True)
        part = jnp.sum(part.astype(F32), axis=0).astype(BF)
        got = swap(part[rows:], C)
        piece = from_slabs(part[:rows], got, pos_back, slab, nz)
        piece = lax.all_to_all(piece, ZH, 0, 0, tiled=True).reshape(nz * rows, -1)
        pieces.append(piece)
        for j in range(1, ny):
            pieces.append(shift(piece, Y, j))
    grad_input = assemble(pieces, pos_back, 2 * slab, nx, ny)

    total = lax.dot_general(
        act_all, grad_hidden, (((0,), (1,)), ((), ())), preferred_element_type=F32
    ).astype(BF)
    total = lax.psum_scatter(total, (Z, X), scatter_dimension=0, tiled=True)
    grad_gate_up = (total.astype(F32) / dp_count).reshape(slab, 2, width)
    return (grad_input, grad_gate_up, grad_down / dp_count)


def solution(mesh):
    split = Mesh(
        mesh.devices.reshape(2, 4, 2, 4, 4), ("dp_0", "dp_1", "dp_2", "tensor_0", "tensor_1")
    )
    return jax.shard_map(
        layer,
        mesh=split,
        in_specs=(
            P(DP, None),
            P(DP, None),
            P(DP, TENSOR),
            P(DP, TENSOR),
            P(DP, None, TENSOR),
            P(DP, TENSOR),
        ),
        out_specs=(P(DP, None), P(DP, None, TENSOR), P(DP, TENSOR)),
        check_vma=False,
    )
```

```python
import functools

import jax
import jax.numpy as jnp
from jax import lax
from jax.experimental import pallas as pl
from jax.experimental.pallas import tpu as pltpu
from jax.sharding import Mesh
from jax.sharding import PartitionSpec as P

Z, X, C = "dp_0", "dp_1", "dp_2"
DP = (Z, X, C)
ZH, Y = "tensor_0", "tensor_1"
TENSOR = (ZH, Y)
BF = jnp.bfloat16
F32 = jnp.float32


def shift(v, axis, step):
    n = lax.axis_size(axis)
    return lax.ppermute(v, axis, [(i, (i + step) % n) for i in range(n)])


def ring(v):
    n = lax.axis_size(X)
    pairs = []
    for i in range(n):
        pairs.append((2 * i, 2 * ((i + 1) % n)))
        pairs.append((2 * i + 1, 2 * ((i - 1) % n) + 1))
    return lax.ppermute(v, (X, C), pairs)


def swap(v, axis):
    return lax.ppermute(v, axis, [(0, 1), (1, 0)])


def to_slabs_kernel(pos_ref, x_ref, mine_ref, theirs_ref, *, slab, nx):
    z = pos_ref[0]
    for core in range(2):
        for odd in range(2):

            @pl.when((pos_ref[1] == core) & (pos_ref[2] == odd))
            def _(core=core, odd=odd):
                for xx in range(nx):
                    q = pos_ref[3 + xx]
                    for ref, side, hops in (
                        (mine_ref, core, q),
                        (theirs_ref, 1 - core, (nx - q) & (nx - 1)),
                    ):
                        for zz in range(2):
                            far = zz ^ z
                            k = 2 * (zz * nx + xx) + side
                            v = x_ref[:, k * slab : (k + 1) * slab]
                            d = (xx + odd) % 2
                            ref[far * (nx // 2) + hops // 2, :, d * slab : (d + 1) * slab] = v


def to_slabs(x, pos, slab, nx):
    tokens, width = x.shape
    rows = 64
    out = jax.ShapeDtypeStruct((nx, tokens, 2 * slab), x.dtype)
    return pl.pallas_call(
        functools.partial(to_slabs_kernel, slab=slab, nx=nx),
        grid_spec=pltpu.PrefetchScalarGridSpec(
            num_scalar_prefetch=1,
            grid=(tokens // rows,),
            in_specs=[pl.BlockSpec((rows, width), lambda i, s: (i, 0))],
            out_specs=[pl.BlockSpec((nx, rows, 2 * slab), lambda i, s: (0, i, 0))] * 2,
        ),
        out_shape=[out, out],
        name="to_slabs",
    )(pos, x)


def to_columns_kernel(pos_ref, x_ref, mine_ref, theirs_ref, *, slab):
    for core in range(2):

        @pl.when(pos_ref[1] == core)
        def _(core=core):
            for k in range(x_ref.shape[1] // (2 * slab)):
                for ref, side in ((mine_ref, core), (theirs_ref, 1 - core)):
                    at = (2 * k + side) * slab
                    ref[:, k * slab : (k + 1) * slab] = x_ref[:, at : at + slab]


def to_columns(x, pos, slab):
    tokens, width = x.shape
    rows = 64
    out = jax.ShapeDtypeStruct((tokens, width // 2), x.dtype)
    return pl.pallas_call(
        functools.partial(to_columns_kernel, slab=slab),
        grid_spec=pltpu.PrefetchScalarGridSpec(
            num_scalar_prefetch=1,
            grid=(tokens // rows,),
            in_specs=[pl.BlockSpec((rows, width), lambda i, s: (i, 0))],
            out_specs=[pl.BlockSpec((rows, width // 2), lambda i, s: (i, 0))] * 2,
        ),
        out_shape=[out, out],
        name="to_columns",
    )(pos, x)


def factors_kernel(g0_ref, g1_ref, u0_ref, u1_ref, hidden_ref, gate_ref, up_ref):
    tokens = g0_ref.shape[1]
    for a, (g_ref, u_ref) in enumerate(((g0_ref, u0_ref), (g1_ref, u1_ref))):
        at = slice(a * tokens, (a + 1) * tokens)
        g = g_ref[...].astype(F32)
        u = u_ref[...].astype(F32)
        s = 1.0 / (1.0 + jnp.exp(-g))
        silu = g * s
        hidden_ref[:, at] = (silu * u).astype(BF)
        gate_ref[:, at] = u * s * (1.0 + g * (1.0 - s))
        up_ref[:, at] = silu


def factors(*args):
    width, tokens = args[0].shape
    outs = [jax.ShapeDtypeStruct((width, 2 * tokens), t) for t in (BF, F32, F32)]
    return pl.pallas_call(factors_kernel, out_shape=outs, name="factors")(*args)


def grad_hidden_kernel(part_ref, got_ref, gate_ref, up_ref, o_ref):
    width, both = part_ref.shape
    tokens = both // 2
    for a in range(2):
        at = slice(a * tokens, (a + 1) * tokens)
        h = part_ref[:, at] + got_ref[:, tokens - a * tokens : both - a * tokens]
        o_ref[:width, at] = (h * gate_ref[:, at]).astype(BF)
        o_ref[width:, at] = (h * up_ref[:, at]).astype(BF)


def grad_hidden_of(part, got, gate, up):
    width, both = part.shape
    return pl.pallas_call(
        grad_hidden_kernel,
        out_shape=jax.ShapeDtypeStruct((2 * width, both), BF),
        name="grad_hidden",
    )(part, got, gate, up)


def cut_kernel(pos_ref, x_ref, *o_refs):
    n = len(o_refs)
    for j, o_ref in enumerate(o_refs):
        at = (pos_ref[3] + j) & (n - 1)
        for a in range(2):
            o_ref[:, a] = x_ref[a, at]


def cut(x, pos, n, m, rows):
    cols = x.shape[1]
    out = jax.ShapeDtypeStruct((m, 2, rows, cols), x.dtype)
    outs = pl.pallas_call(
        cut_kernel,
        in_specs=[
            pl.BlockSpec(memory_space=pltpu.SMEM),
            pl.BlockSpec(memory_space=pltpu.VMEM),
        ],
        out_shape=[out] * n,
        name="cut",
    )(pos, x.reshape(2, n, m, rows, cols))
    return [o.reshape(m * 2 * rows, cols) for o in outs]


def from_slabs_kernel(pos_ref, own_ref, other_ref, o_ref, *, slab):
    core_odd = pos_ref[1] == 1
    own, other = own_ref[...], other_ref[...]
    for i in range(own.shape[1] // slab):
        mine, theirs = (v[:, i * slab : (i + 1) * slab] for v in (own, other))
        even = jnp.where(core_odd, theirs, mine)
        odd = jnp.where(core_odd, mine, theirs)
        both = jnp.concatenate([even, odd], axis=1)
        o_ref[:, 2 * i * slab : 2 * (i + 1) * slab] = both


def from_slabs(own, other, pos, slab):
    rows, cols = own.shape
    vmem = pl.BlockSpec(memory_space=pltpu.VMEM)
    return pl.pallas_call(
        functools.partial(from_slabs_kernel, slab=slab),
        in_specs=[pl.BlockSpec(memory_space=pltpu.SMEM), vmem, vmem],
        out_shape=jax.ShapeDtypeStruct((rows, 2 * cols), own.dtype),
        name="from_slabs",
    )(pos, own, other)


def assemble_kernel(pos_ref, *refs, block, nx, ny):
    o_ref = refs[-1]
    zi, xi, yi = pos_ref[0], pos_ref[2], pos_ref[3]
    rows = refs[0].shape[0]
    for n in range(nx // 2):
        for j in range(ny):
            ref = refs[n * ny + j]
            row = pl.multiple_of(((yi - j) & (ny - 1)) * rows, rows)
            for i in range(2):
                q = 2 * n + i
                for d, at in enumerate((zi * nx + ((xi - q) & (nx - 1)), (1 - zi) * nx + ((xi + q) & (nx - 1)))):
                    src = (2 * i + d) * block
                    o_ref[pl.ds(row, rows), pl.ds(pl.multiple_of(at * block, 128), block)] = ref[
                        :, src : src + block
                    ]


def assemble(pieces, pos, block, nx, ny):
    rows, cols = pieces[0].shape
    vmem = pl.BlockSpec(memory_space=pltpu.VMEM)
    return pl.pallas_call(
        functools.partial(assemble_kernel, block=block, nx=nx, ny=ny),
        in_specs=[pl.BlockSpec(memory_space=pltpu.SMEM)] + [vmem] * len(pieces),
        out_shape=jax.ShapeDtypeStruct((ny * rows, (nx // 2) * cols), pieces[0].dtype),
        name="assemble",
    )(pos, *pieces)


def layer(activations, grad_out, gate_pre, up_pre, gate_up, down_weight):
    tokens = activations.shape[0]
    slab, width = down_weight.shape
    nx, ny, nz = lax.axis_size(X), lax.axis_size(Y), lax.axis_size(ZH)
    dp_count = lax.axis_size(DP)
    rows = tokens // (ny * nz)
    xi, zi, ci = lax.axis_index(X), lax.axis_index(Z), lax.axis_index(C)
    yi = lax.axis_index(Y)
    sign = 2 * ci - 1
    pos = jnp.stack(
        [zi, ci, xi & 1] + [(sign * (k - xi)) & (nx - 1) for k in range(nx)]
    ).astype(jnp.int32)
    pos_back = jnp.stack([zi, ci, xi, yi]).astype(jnp.int32)

    near, far = [down_weight], []
    far.append(swap(down_weight, Z))
    for _ in range(1, nx):
        near.append(ring(near[-1]))
        far.append(ring(far[-1]))
    gate_near = gate_up.reshape(slab, 2 * width)
    gate_far = [swap(gate_near, Z)]
    gate_near = [gate_near]
    for _ in range(1, nx):
        gate_near.append(shift(gate_near[-1], X, 1))
        gate_far.append(shift(gate_far[-1], X, -1))

    out_mine, out_theirs = to_slabs(grad_out, pos, slab, nx)
    out_theirs = swap(out_theirs, C)
    out_all = jnp.concatenate([out_mine, out_theirs], axis=1)
    gate_other = swap(gate_pre.T, C)
    up_other = swap(up_pre.T, C)
    hidden, gate_factor, up_factor = factors(gate_pre.T, gate_other, up_pre.T, up_other)
    act_mine, act_theirs = to_columns(activations, pos, slab)
    act_theirs = swap(act_theirs, C)
    act_all = jnp.concatenate([act_mine, act_theirs])

    part_h = None
    for k, pieces in ((0, near[:2]), (2, far[:2]), (1, near[2:]), (3, far[2:])):
        p = lax.dot_general(
            jnp.concatenate(pieces),
            out_all[k],
            (((0,), (1,)), ((), ())),
            preferred_element_type=F32,
        )
        part_h = p if part_h is None else part_h + p
    got_h = swap(part_h, C)
    grad_hidden = grad_hidden_of(part_h, got_h, gate_factor, up_factor)

    def down_block(k):
        return lax.dot_general(
            out_all[k], hidden, (((0,), (1,)), ((), ())), preferred_element_type=F32
        )

    sums = []
    for k in (0, 1):
        got = swap(down_block(2 + k).astype(BF), Z)
        both = down_block(k) + got.astype(F32)
        sums += [both[:slab], both[slab:]]
    grad_down = sums[1]
    for q in (2, 3, 0):
        grad_down = sums[q] + ring(grad_down.astype(BF)).astype(F32)

    pieces = []
    for n in range(2):
        w = jnp.concatenate(
            [g[q] for q in (2 * n, 2 * n + 1) for g in (gate_near, gate_far)]
        )
        part = lax.dot_general(
            grad_hidden, w, (((0,), (1,)), ((), ())), preferred_element_type=F32
        ).astype(BF)
        blocks = cut(part, pos_back, ny, nz, rows)
        part = blocks[0].astype(F32)
        for j in range(1, ny):
            got = shift(blocks[j], Y, j)
            part = part + got.astype(F32)
        part = part.astype(BF).reshape(nz, 2 * rows, -1)
        part = lax.all_to_all(part, ZH, 0, 0, tiled=True)
        part = jnp.sum(part.astype(F32), axis=0).astype(BF)
        got = swap(part[rows:], C)
        piece = from_slabs(part[:rows], got, pos_back, slab)
        piece = lax.all_gather(piece, ZH, axis=0, tiled=True)
        pieces.append(piece)
        for j in range(1, ny):
            pieces.append(shift(piece, Y, j))
    grad_input = assemble(pieces, pos_back, 2 * slab, nx, ny)

    total = lax.dot_general(
        act_all, grad_hidden, (((0,), (1,)), ((), ())), preferred_element_type=F32
    ).astype(BF)
    total = lax.psum_scatter(total, (Z, X), scatter_dimension=0, tiled=True)
    grad_gate_up = (total.astype(F32) / dp_count).reshape(slab, 2, width)
    return (grad_input, grad_gate_up, grad_down / dp_count)


def solution(mesh):
    split = Mesh(
        mesh.devices.reshape(2, 4, 2, 4, 4), ("dp_0", "dp_1", "dp_2", "tensor_0", "tensor_1")
    )
    return jax.shard_map(
        layer,
        mesh=split,
        in_specs=(
            P(DP, None),
            P(DP, None),
            P(DP, TENSOR),
            P(DP, TENSOR),
            P(DP, None, TENSOR),
            P(DP, TENSOR),
        ),
        out_specs=(P(DP, None), P(DP, None, TENSOR), P(DP, TENSOR)),
        check_vma=False,
    )
```

```python
import functools

import jax
import jax.numpy as jnp
from jax import lax
from jax.experimental import pallas as pl
from jax.experimental.pallas import tpu as pltpu
from jax.sharding import Mesh
from jax.sharding import PartitionSpec as P

Z, X, C = "dp_0", "dp_1", "dp_2"
DP = (Z, X, C)
ZH, Y = "tensor_0", "tensor_1"
TENSOR = (ZH, Y)
BF = jnp.bfloat16
F32 = jnp.float32


def shift(v, axis, step):
    n = lax.axis_size(axis)
    return lax.ppermute(v, axis, [(i, (i + step) % n) for i in range(n)])


def ring(v):
    n = lax.axis_size(X)
    pairs = []
    for i in range(n):
        pairs.append((2 * i, 2 * ((i + 1) % n)))
        pairs.append((2 * i + 1, 2 * ((i - 1) % n) + 1))
    return lax.ppermute(v, (X, C), pairs)


def swap(v, axis):
    return lax.ppermute(v, axis, [(0, 1), (1, 0)])


def to_columns_kernel(pos_ref, x_ref, mine_ref, theirs_ref, *, slab):
    for core in range(2):

        @pl.when(pos_ref[1] == core)
        def _(core=core):
            for k in range(x_ref.shape[1] // (2 * slab)):
                for ref, side in ((mine_ref, core), (theirs_ref, 1 - core)):
                    at = (2 * k + side) * slab
                    ref[:, k * slab : (k + 1) * slab] = x_ref[:, at : at + slab]


def to_columns(x, pos, slab):
    tokens, width = x.shape
    rows = 64
    out = jax.ShapeDtypeStruct((tokens, width // 2), x.dtype)
    return pl.pallas_call(
        functools.partial(to_columns_kernel, slab=slab),
        grid_spec=pltpu.PrefetchScalarGridSpec(
            num_scalar_prefetch=1,
            grid=(tokens // rows,),
            in_specs=[pl.BlockSpec((rows, width), lambda i, s: (i, 0))],
            out_specs=[pl.BlockSpec((rows, width // 2), lambda i, s: (i, 0))] * 2,
        ),
        out_shape=[out, out],
        name="to_columns",
    )(pos, x)


def factors_kernel(g0_ref, g1_ref, u0_ref, u1_ref, hidden_ref, gate_ref, up_ref):
    tokens = g0_ref.shape[1]
    for a, (g_ref, u_ref) in enumerate(((g0_ref, u0_ref), (g1_ref, u1_ref))):
        at = slice(a * tokens, (a + 1) * tokens)
        g = g_ref[...].astype(F32)
        u = u_ref[...].astype(F32)
        s = 1.0 / (1.0 + jnp.exp(-g))
        silu = g * s
        hidden_ref[:, at] = (silu * u).astype(BF)
        gate_ref[:, at] = u * s * (1.0 + g * (1.0 - s))
        up_ref[:, at] = silu


def factors(*args):
    width, tokens = args[0].shape
    outs = [jax.ShapeDtypeStruct((width, 2 * tokens), t) for t in (BF, F32, F32)]
    return pl.pallas_call(factors_kernel, out_shape=outs, name="factors")(*args)


def grad_hidden_kernel(part_ref, got_ref, gate_ref, up_ref, o_ref):
    width, both = part_ref.shape
    tokens = both // 2
    for a in range(2):
        at = slice(a * tokens, (a + 1) * tokens)
        h = part_ref[:, at] + got_ref[:, tokens - a * tokens : both - a * tokens]
        o_ref[:width, at] = (h * gate_ref[:, at]).astype(BF)
        o_ref[width:, at] = (h * up_ref[:, at]).astype(BF)


def grad_hidden_of(part, got, gate, up):
    width, both = part.shape
    return pl.pallas_call(
        grad_hidden_kernel,
        out_shape=jax.ShapeDtypeStruct((2 * width, both), BF),
        name="grad_hidden",
    )(part, got, gate, up)


def cut_kernel(pos_ref, x_ref, *o_refs):
    n = len(o_refs)
    for j, o_ref in enumerate(o_refs):
        at = (pos_ref[3] + j) & (n - 1)
        for a in range(2):
            o_ref[:, a] = x_ref[a, at]


def cut(x, pos, n, m, rows):
    cols = x.shape[1]
    out = jax.ShapeDtypeStruct((m, 2, rows, cols), x.dtype)
    outs = pl.pallas_call(
        cut_kernel,
        in_specs=[
            pl.BlockSpec(memory_space=pltpu.SMEM),
            pl.BlockSpec(memory_space=pltpu.VMEM),
        ],
        out_shape=[out] * n,
        name="cut",
    )(pos, x.reshape(2, n, m, rows, cols))
    return [o.reshape(m * 2 * rows, cols) for o in outs]


def from_slabs_kernel(pos_ref, own_ref, other_ref, o_ref, *, slab):
    core_odd = pos_ref[1] == 1
    own, other = own_ref[...], other_ref[...]
    for i in range(own.shape[1] // slab):
        mine, theirs = (v[:, i * slab : (i + 1) * slab] for v in (own, other))
        even = jnp.where(core_odd, theirs, mine)
        odd = jnp.where(core_odd, mine, theirs)
        both = jnp.concatenate([even, odd], axis=1)
        o_ref[:, 2 * i * slab : 2 * (i + 1) * slab] = both


def from_slabs(own, other, pos, slab):
    rows, cols = own.shape
    vmem = pl.BlockSpec(memory_space=pltpu.VMEM)
    return pl.pallas_call(
        functools.partial(from_slabs_kernel, slab=slab),
        in_specs=[pl.BlockSpec(memory_space=pltpu.SMEM), vmem, vmem],
        out_shape=jax.ShapeDtypeStruct((rows, 2 * cols), own.dtype),
        name="from_slabs",
    )(pos, own, other)


def assemble_kernel(pos_ref, *refs, block, nx, ny):
    o_ref = refs[-1]
    zi, xi, yi = pos_ref[0], pos_ref[2], pos_ref[3]
    rows = refs[0].shape[0]
    for n in range(nx // 2):
        for j in range(ny):
            ref = refs[n * ny + j]
            row = pl.multiple_of(((yi - j) & (ny - 1)) * rows, rows)
            for i in range(2):
                q = 2 * n + i
                for d, at in enumerate((zi * nx + ((xi - q) & (nx - 1)), (1 - zi) * nx + ((xi + q) & (nx - 1)))):
                    src = (2 * i + d) * block
                    o_ref[pl.ds(row, rows), pl.ds(pl.multiple_of(at * block, 128), block)] = ref[
                        :, src : src + block
                    ]


def assemble(pieces, pos, block, nx, ny):
    rows, cols = pieces[0].shape
    vmem = pl.BlockSpec(memory_space=pltpu.VMEM)
    return pl.pallas_call(
        functools.partial(assemble_kernel, block=block, nx=nx, ny=ny),
        in_specs=[pl.BlockSpec(memory_space=pltpu.SMEM)] + [vmem] * len(pieces),
        out_shape=jax.ShapeDtypeStruct((ny * rows, (nx // 2) * cols), pieces[0].dtype),
        name="assemble",
    )(pos, *pieces)


def layer(activations, grad_out, gate_pre, up_pre, gate_up, down_weight):
    tokens = activations.shape[0]
    slab, width = down_weight.shape
    nx, ny, nz = lax.axis_size(X), lax.axis_size(Y), lax.axis_size(ZH)
    dp_count = lax.axis_size(DP)
    rows = tokens // (ny * nz)
    xi, zi, ci = lax.axis_index(X), lax.axis_index(Z), lax.axis_index(C)
    yi = lax.axis_index(Y)
    sign = 2 * ci - 1
    pos = jnp.stack([zi, ci, xi, yi]).astype(jnp.int32)

    near, far = [down_weight], []
    far.append(swap(down_weight, Z))
    for _ in range(1, nx):
        near.append(ring(near[-1]))
        far.append(ring(far[-1]))
    gate_near = gate_up.reshape(slab, 2 * width)
    gate_far = [swap(gate_near, Z)]
    gate_near = [gate_near]
    for _ in range(1, nx):
        gate_near.append(shift(gate_near[-1], X, 1))
        gate_far.append(shift(gate_far[-1], X, -1))

    out_mine, out_theirs = to_columns(grad_out, pos, slab)
    out_theirs = swap(out_theirs, C)
    out_all = jnp.concatenate([out_mine, out_theirs])
    gate_other = swap(gate_pre.T, C)
    up_other = swap(up_pre.T, C)
    hidden, gate_factor, up_factor = factors(gate_pre.T, gate_other, up_pre.T, up_other)
    act_mine, act_theirs = to_columns(activations, pos, slab)
    act_theirs = swap(act_theirs, C)
    act_all = jnp.concatenate([act_mine, act_theirs])

    down = jnp.zeros((2 * nx, slab, width), BF)
    for h in range(nx):
        x = (xi + sign * h) & (nx - 1)
        down = lax.dynamic_update_slice(down, near[h][None], (zi * nx + x, 0, 0))
        down = lax.dynamic_update_slice(down, far[h][None], ((1 - zi) * nx + x, 0, 0))
    down = down.reshape(2 * nx * slab, width)
    part_h = lax.dot_general(down, out_all, (((0,), (1,)), ((), ())), preferred_element_type=F32)
    got_h = swap(part_h, C)
    grad_hidden = grad_hidden_of(part_h, got_h, gate_factor, up_factor)

    pieces = []
    for n in range(2):
        w = jnp.concatenate(
            [g[q] for q in (2 * n, 2 * n + 1) for g in (gate_near, gate_far)]
        )
        part = lax.dot_general(
            grad_hidden, w, (((0,), (1,)), ((), ())), preferred_element_type=F32
        ).astype(BF)
        blocks = cut(part, pos, ny, nz, rows)
        part = blocks[0].astype(F32)
        for j in range(1, ny):
            got = shift(blocks[j], Y, j)
            part = part + got.astype(F32)
        part = part.astype(BF).reshape(nz, 2 * rows, -1)
        part = lax.all_to_all(part, ZH, 0, 0, tiled=True)
        part = jnp.sum(part.astype(F32), axis=0).astype(BF)
        got = swap(part[rows:], C)
        piece = from_slabs(part[:rows], got, pos, slab)
        piece = lax.all_gather(piece, ZH, axis=0, tiled=True)
        pieces.append(piece)
        for j in range(1, ny):
            pieces.append(shift(piece, Y, j))
    grad_input = assemble(pieces, pos, 2 * slab, nx, ny)

    grad_down = lax.dot_general(
        out_all, hidden, (((0,), (1,)), ((), ())), preferred_element_type=F32
    ).astype(BF)
    grad_down = lax.psum_scatter(grad_down, (Z, X), scatter_dimension=0, tiled=True)
    grad_down = grad_down.astype(F32) / dp_count
    total = lax.dot_general(
        act_all, grad_hidden, (((0,), (1,)), ((), ())), preferred_element_type=F32
    ).astype(BF)
    total = lax.psum_scatter(total, (Z, X), scatter_dimension=0, tiled=True)
    grad_gate_up = (total.astype(F32) / dp_count).reshape(slab, 2, width)
    return (grad_input, grad_gate_up, grad_down)


def solution(mesh):
    split = Mesh(
        mesh.devices.reshape(2, 4, 2, 4, 4), ("dp_0", "dp_1", "dp_2", "tensor_0", "tensor_1")
    )
    return jax.shard_map(
        layer,
        mesh=split,
        in_specs=(
            P(DP, None),
            P(DP, None),
            P(DP, TENSOR),
            P(DP, TENSOR),
            P(DP, None, TENSOR),
            P(DP, TENSOR),
        ),
        out_specs=(P(DP, None), P(DP, None, TENSOR), P(DP, TENSOR)),
        check_vma=False,
    )
```

```python
import functools

import jax
import jax.numpy as jnp
from jax import lax
from jax.experimental import pallas as pl
from jax.experimental.pallas import tpu as pltpu
from jax.sharding import Mesh
from jax.sharding import PartitionSpec as P

Z, X, C = "dp_0", "dp_1", "dp_2"
DP = (Z, X, C)
ZH, Y = "tensor_0", "tensor_1"
TENSOR = (ZH, Y)
BF = jnp.bfloat16
F32 = jnp.float32


def shift(v, axis, step):
    n = lax.axis_size(axis)
    return lax.ppermute(v, axis, [(i, (i + step) % n) for i in range(n)])


def ring(v):
    n = lax.axis_size(X)
    pairs = []
    for i in range(n):
        pairs.append((2 * i, 2 * ((i + 1) % n)))
        pairs.append((2 * i + 1, 2 * ((i - 1) % n) + 1))
    return lax.ppermute(v, (X, C), pairs)


def swap(v, axis):
    return lax.ppermute(v, axis, [(0, 1), (1, 0)])


def to_columns_kernel(pos_ref, x_ref, mine_ref, theirs_ref, *, slab):
    for core in range(2):

        @pl.when(pos_ref[1] == core)
        def _(core=core):
            for k in range(x_ref.shape[1] // (2 * slab)):
                for ref, side in ((mine_ref, core), (theirs_ref, 1 - core)):
                    at = (2 * k + side) * slab
                    ref[:, k * slab : (k + 1) * slab] = x_ref[:, at : at + slab]


def to_columns(x, pos, slab):
    tokens, width = x.shape
    rows = 64
    out = jax.ShapeDtypeStruct((tokens, width // 2), x.dtype)
    return pl.pallas_call(
        functools.partial(to_columns_kernel, slab=slab),
        grid_spec=pltpu.PrefetchScalarGridSpec(
            num_scalar_prefetch=1,
            grid=(tokens // rows,),
            in_specs=[pl.BlockSpec((rows, width), lambda i, s: (i, 0))],
            out_specs=[pl.BlockSpec((rows, width // 2), lambda i, s: (i, 0))] * 2,
        ),
        out_shape=[out, out],
        name="to_columns",
    )(pos, x)


def in_chip_order_kernel(pos_ref, *refs):
    o_ref = refs[-1]
    n = (len(refs) - 1) // 2
    z, x = pos_ref[0], pos_ref[2]
    sign = 2 * pos_ref[1] - 1
    for h in range(n):
        at = (x + sign * h) & (n - 1)
        o_ref[z * n + at] = refs[h][...]
        o_ref[(1 - z) * n + at] = refs[n + h][...]


def in_chip_order(near, far, pos):
    n = len(near)
    slab, width = near[0].shape
    out = pl.pallas_call(
        in_chip_order_kernel,
        in_specs=[pl.BlockSpec(memory_space=pltpu.SMEM)]
        + [pl.BlockSpec(memory_space=pltpu.VMEM)] * (2 * n),
        out_shape=jax.ShapeDtypeStruct((2 * n, slab, width), near[0].dtype),
        name="in_chip_order",
    )(pos, *near, *far)
    return out.reshape(2 * n * slab, width)


def factors_kernel(g0_ref, g1_ref, u0_ref, u1_ref, hidden_ref, gate_ref, up_ref):
    tokens = g0_ref.shape[1]
    for a, (g_ref, u_ref) in enumerate(((g0_ref, u0_ref), (g1_ref, u1_ref))):
        at = slice(a * tokens, (a + 1) * tokens)
        g = g_ref[...].astype(F32)
        u = u_ref[...].astype(F32)
        s = 1.0 / (1.0 + jnp.exp(-g))
        silu = g * s
        hidden_ref[:, at] = (silu * u).astype(BF)
        gate_ref[:, at] = u * s * (1.0 + g * (1.0 - s))
        up_ref[:, at] = silu


def factors(*args):
    width, tokens = args[0].shape
    outs = [jax.ShapeDtypeStruct((width, 2 * tokens), t) for t in (BF, F32, F32)]
    return pl.pallas_call(factors_kernel, out_shape=outs, name="factors")(*args)


def grad_hidden_kernel(part_ref, got_ref, gate_ref, up_ref, o_ref):
    width, both = part_ref.shape
    tokens = both // 2
    for a in range(2):
        at = slice(a * tokens, (a + 1) * tokens)
        h = part_ref[:, at] + got_ref[:, tokens - a * tokens : both - a * tokens]
        o_ref[:width, at] = (h * gate_ref[:, at]).astype(BF)
        o_ref[width:, at] = (h * up_ref[:, at]).astype(BF)


def grad_hidden_of(part, got, gate, up):
    width, both = part.shape
    return pl.pallas_call(
        grad_hidden_kernel,
        out_shape=jax.ShapeDtypeStruct((2 * width, both), BF),
        name="grad_hidden",
    )(part, got, gate, up)


def cut_kernel(pos_ref, x_ref, *o_refs):
    n = len(o_refs)
    for j, o_ref in enumerate(o_refs):
        at = (pos_ref[3] + j) & (n - 1)
        for a in range(2):
            o_ref[:, a] = x_ref[a, at]


def cut(x, pos, n, m, rows):
    cols = x.shape[1]
    out = jax.ShapeDtypeStruct((m, 2, rows, cols), x.dtype)
    outs = pl.pallas_call(
        cut_kernel,
        in_specs=[
            pl.BlockSpec(memory_space=pltpu.SMEM),
            pl.BlockSpec(memory_space=pltpu.VMEM),
        ],
        out_shape=[out] * n,
        name="cut",
    )(pos, x.reshape(2, n, m, rows, cols))
    return [o.reshape(m * 2 * rows, cols) for o in outs]


def from_slabs_kernel(pos_ref, own_ref, other_ref, o_ref, *, slab):
    core_odd = pos_ref[1] == 1
    own, other = own_ref[...], other_ref[...]
    for i in range(own.shape[1] // slab):
        mine, theirs = (v[:, i * slab : (i + 1) * slab] for v in (own, other))
        even = jnp.where(core_odd, theirs, mine)
        odd = jnp.where(core_odd, mine, theirs)
        both = jnp.concatenate([even, odd], axis=1)
        o_ref[:, 2 * i * slab : 2 * (i + 1) * slab] = both


def from_slabs(own, other, pos, slab):
    rows, cols = own.shape
    vmem = pl.BlockSpec(memory_space=pltpu.VMEM)
    return pl.pallas_call(
        functools.partial(from_slabs_kernel, slab=slab),
        in_specs=[pl.BlockSpec(memory_space=pltpu.SMEM), vmem, vmem],
        out_shape=jax.ShapeDtypeStruct((rows, 2 * cols), own.dtype),
        name="from_slabs",
    )(pos, own, other)


def assemble_kernel(pos_ref, *refs, block, nx, ny):
    o_ref = refs[-1]
    zi, xi, yi = pos_ref[0], pos_ref[2], pos_ref[3]
    rows = refs[0].shape[0]
    for n in range(nx // 2):
        for j in range(ny):
            ref = refs[n * ny + j]
            row = pl.multiple_of(((yi - j) & (ny - 1)) * rows, rows)
            for i in range(2):
                q = 2 * n + i
                for d, at in enumerate((zi * nx + ((xi - q) & (nx - 1)), (1 - zi) * nx + ((xi + q) & (nx - 1)))):
                    src = (2 * i + d) * block
                    o_ref[pl.ds(row, rows), pl.ds(pl.multiple_of(at * block, 128), block)] = ref[
                        :, src : src + block
                    ]


def assemble(pieces, pos, block, nx, ny):
    rows, cols = pieces[0].shape
    vmem = pl.BlockSpec(memory_space=pltpu.VMEM)
    return pl.pallas_call(
        functools.partial(assemble_kernel, block=block, nx=nx, ny=ny),
        in_specs=[pl.BlockSpec(memory_space=pltpu.SMEM)] + [vmem] * len(pieces),
        out_shape=jax.ShapeDtypeStruct((ny * rows, (nx // 2) * cols), pieces[0].dtype),
        name="assemble",
    )(pos, *pieces)


def layer(activations, grad_out, gate_pre, up_pre, gate_up, down_weight):
    tokens = activations.shape[0]
    slab, width = down_weight.shape
    nx, ny, nz = lax.axis_size(X), lax.axis_size(Y), lax.axis_size(ZH)
    dp_count = lax.axis_size(DP)
    rows = tokens // (ny * nz)
    xi, zi, ci = lax.axis_index(X), lax.axis_index(Z), lax.axis_index(C)
    yi = lax.axis_index(Y)
    pos = jnp.stack([zi, ci, xi, yi]).astype(jnp.int32)

    near, far = [down_weight], []
    far.append(swap(down_weight, Z))
    for _ in range(1, nx):
        near.append(ring(near[-1]))
        far.append(ring(far[-1]))
    gate_near = gate_up.reshape(slab, 2 * width)
    gate_far = [swap(gate_near, Z)]
    gate_near = [gate_near] + [None] * (nx - 1)
    gate_far = gate_far + [None] * (nx - 1)
    for h, v, step in ((1, 0, 1), (nx - 1, 0, -1), (2, 1, 1)):
        gate_near[h] = shift(gate_near[v], X, step)
        gate_far[h] = shift(gate_far[v], X, -step)

    out_mine, out_theirs = to_columns(grad_out, pos, slab)
    out_theirs = swap(out_theirs, C)
    out_all = jnp.concatenate([out_mine, out_theirs])
    gate_other = swap(gate_pre.T, C)
    up_other = swap(up_pre.T, C)
    hidden, gate_factor, up_factor = factors(gate_pre.T, gate_other, up_pre.T, up_other)
    act_mine, act_theirs = to_columns(activations, pos, slab)
    act_theirs = swap(act_theirs, C)
    act_all = jnp.concatenate([act_mine, act_theirs])

    down = in_chip_order(near, far, pos)
    part_h = lax.dot_general(down, out_all, (((0,), (1,)), ((), ())), preferred_element_type=F32)
    got_h = swap(part_h, C)
    grad_hidden = grad_hidden_of(part_h, got_h, gate_factor, up_factor)

    pieces = []
    for n in range(2):
        w = jnp.concatenate(
            [g[q] for q in (2 * n, 2 * n + 1) for g in (gate_near, gate_far)]
        )
        part = lax.dot_general(
            grad_hidden, w, (((0,), (1,)), ((), ())), preferred_element_type=F32
        ).astype(BF)
        blocks = cut(part, pos, ny, nz, rows)
        part = blocks[0].astype(F32)
        for j in range(1, ny):
            got = shift(blocks[j], Y, j)
            part = part + got.astype(F32)
        part = part.astype(BF).reshape(nz, 2 * rows, -1)
        part = lax.all_to_all(part, ZH, 0, 0, tiled=True)
        part = jnp.sum(part.astype(F32), axis=0).astype(BF)
        got = swap(part[rows:], C)
        piece = from_slabs(part[:rows], got, pos, slab)
        piece = lax.all_gather(piece, ZH, axis=0, tiled=True)
        pieces.append(piece)
        for j in range(1, ny):
            pieces.append(shift(piece, Y, j))
    grad_input = assemble(pieces, pos, 2 * slab, nx, ny)

    grad_down = lax.dot_general(
        out_all, hidden, (((0,), (1,)), ((), ())), preferred_element_type=F32
    ).astype(BF)
    grad_down = lax.psum_scatter(grad_down, (Z, X), scatter_dimension=0, tiled=True)
    grad_down = grad_down.astype(F32) / dp_count
    total = lax.dot_general(
        act_all, grad_hidden, (((0,), (1,)), ((), ())), preferred_element_type=F32
    ).astype(BF)
    total = lax.psum_scatter(total, (Z, X), scatter_dimension=0, tiled=True)
    grad_gate_up = (total.astype(F32) / dp_count).reshape(slab, 2, width)
    return (grad_input, grad_gate_up, grad_down)


def solution(mesh):
    split = Mesh(
        mesh.devices.reshape(2, 4, 2, 4, 4), ("dp_0", "dp_1", "dp_2", "tensor_0", "tensor_1")
    )
    return jax.shard_map(
        layer,
        mesh=split,
        in_specs=(
            P(DP, None),
            P(DP, None),
            P(DP, TENSOR),
            P(DP, TENSOR),
            P(DP, None, TENSOR),
            P(DP, TENSOR),
        ),
        out_specs=(P(DP, None), P(DP, None, TENSOR), P(DP, TENSOR)),
        check_vma=False,
    )
```

```python
import functools

import jax
import jax.numpy as jnp
from jax import lax
from jax.experimental import pallas as pl
from jax.experimental.pallas import tpu as pltpu
from jax.sharding import Mesh
from jax.sharding import PartitionSpec as P

Z, X, C = "dp_0", "dp_1", "dp_2"
DP = (Z, X, C)
ZH, Y = "tensor_0", "tensor_1"
TENSOR = (ZH, Y)
BF = jnp.bfloat16
F32 = jnp.float32


def shift(v, axis, step):
    n = lax.axis_size(axis)
    return lax.ppermute(v, axis, [(i, (i + step) % n) for i in range(n)])


def ring(v):
    n = lax.axis_size(X)
    pairs = []
    for i in range(n):
        pairs.append((2 * i, 2 * ((i + 1) % n)))
        pairs.append((2 * i + 1, 2 * ((i - 1) % n) + 1))
    return lax.ppermute(v, (X, C), pairs)


def swap(v, axis):
    return lax.ppermute(v, axis, [(0, 1), (1, 0)])


def to_columns_kernel(pos_ref, x_ref, mine_ref, theirs_ref, *, slab):
    for core in range(2):

        @pl.when(pos_ref[1] == core)
        def _(core=core):
            for k in range(x_ref.shape[1] // (2 * slab)):
                for ref, side in ((mine_ref, core), (theirs_ref, 1 - core)):
                    at = (2 * k + side) * slab
                    ref[:, k * slab : (k + 1) * slab] = x_ref[:, at : at + slab]


def to_columns(x, pos, slab):
    tokens, width = x.shape
    rows = 64
    out = jax.ShapeDtypeStruct((tokens, width // 2), x.dtype)
    return pl.pallas_call(
        functools.partial(to_columns_kernel, slab=slab),
        grid_spec=pltpu.PrefetchScalarGridSpec(
            num_scalar_prefetch=1,
            grid=(tokens // rows,),
            in_specs=[pl.BlockSpec((rows, width), lambda i, s: (i, 0))],
            out_specs=[pl.BlockSpec((rows, width // 2), lambda i, s: (i, 0))] * 2,
        ),
        out_shape=[out, out],
        name="to_columns",
    )(pos, x)


def factors_kernel(own_ref, other_ref, hidden_ref, gate_ref, up_ref):
    width = hidden_ref.shape[0]
    tokens = own_ref.shape[1]
    for a, ref in enumerate((own_ref, other_ref)):
        at = slice(a * tokens, (a + 1) * tokens)
        g = ref[:width].astype(F32)
        u = ref[width:].astype(F32)
        s = 1.0 / (1.0 + jnp.exp(-g))
        silu = g * s
        hidden_ref[:, at] = (silu * u).astype(BF)
        gate_ref[:, at] = u * s * (1.0 + g * (1.0 - s))
        up_ref[:, at] = silu


def factors(own, other):
    width, tokens = own.shape
    outs = [jax.ShapeDtypeStruct((width // 2, 2 * tokens), t) for t in (BF, F32, F32)]
    return pl.pallas_call(factors_kernel, out_shape=outs, name="factors")(own, other)


def grad_hidden_kernel(part_ref, got_ref, gate_ref, up_ref, o_ref):
    width, both = part_ref.shape
    tokens = both // 2
    for a in range(2):
        at = slice(a * tokens, (a + 1) * tokens)
        h = part_ref[:, at] + got_ref[:, tokens - a * tokens : both - a * tokens]
        o_ref[:width, at] = (h * gate_ref[:, at]).astype(BF)
        o_ref[width:, at] = (h * up_ref[:, at]).astype(BF)


def grad_hidden_of(part, got, gate, up):
    width, both = part.shape
    return pl.pallas_call(
        grad_hidden_kernel,
        out_shape=jax.ShapeDtypeStruct((2 * width, both), BF),
        name="grad_hidden",
    )(part, got, gate, up)


def cut_kernel(pos_ref, x_ref, *o_refs):
    n = len(o_refs)
    for j, o_ref in enumerate(o_refs):
        at = (pos_ref[3] + j) & (n - 1)
        for a in range(2):
            o_ref[:, a] = x_ref[a, at]


def cut(x, pos, n, m, rows):
    cols = x.shape[1]
    out = jax.ShapeDtypeStruct((m, 2, rows, cols), x.dtype)
    outs = pl.pallas_call(
        cut_kernel,
        in_specs=[
            pl.BlockSpec(memory_space=pltpu.SMEM),
            pl.BlockSpec(memory_space=pltpu.VMEM),
        ],
        out_shape=[out] * n,
        name="cut",
    )(pos, x.reshape(2, n, m, rows, cols))
    return [o.reshape(m * 2 * rows, cols) for o in outs]


def from_slabs_kernel(pos_ref, own_ref, other_ref, o_ref, *, slab):
    core_odd = pos_ref[1] == 1
    own, other = own_ref[...], other_ref[...]
    for i in range(own.shape[1] // slab):
        mine, theirs = (v[:, i * slab : (i + 1) * slab] for v in (own, other))
        even = jnp.where(core_odd, theirs, mine)
        odd = jnp.where(core_odd, mine, theirs)
        both = jnp.concatenate([even, odd], axis=1)
        o_ref[:, 2 * i * slab : 2 * (i + 1) * slab] = both


def from_slabs(own, other, pos, slab):
    rows, cols = own.shape
    vmem = pl.BlockSpec(memory_space=pltpu.VMEM)
    return pl.pallas_call(
        functools.partial(from_slabs_kernel, slab=slab),
        in_specs=[pl.BlockSpec(memory_space=pltpu.SMEM), vmem, vmem],
        out_shape=jax.ShapeDtypeStruct((rows, 2 * cols), own.dtype),
        name="from_slabs",
    )(pos, own, other)


def assemble_kernel(pos_ref, *refs, block, nx, ny):
    o_ref = refs[-1]
    zi, xi, yi = pos_ref[0], pos_ref[2], pos_ref[3]
    rows = refs[0].shape[0]
    for n in range(nx // 2):
        for j in range(ny):
            ref = refs[n * ny + j]
            row = pl.multiple_of(((yi - j) & (ny - 1)) * rows, rows)
            for i in range(2):
                q = 2 * n + i
                for d, at in enumerate((zi * nx + ((xi - q) & (nx - 1)), (1 - zi) * nx + ((xi + q) & (nx - 1)))):
                    src = (2 * i + d) * block
                    o_ref[pl.ds(row, rows), pl.ds(pl.multiple_of(at * block, 128), block)] = ref[
                        :, src : src + block
                    ]


def assemble(pieces, pos, block, nx, ny):
    rows, cols = pieces[0].shape
    vmem = pl.BlockSpec(memory_space=pltpu.VMEM)
    return pl.pallas_call(
        functools.partial(assemble_kernel, block=block, nx=nx, ny=ny),
        in_specs=[pl.BlockSpec(memory_space=pltpu.SMEM)] + [vmem] * len(pieces),
        out_shape=jax.ShapeDtypeStruct((ny * rows, (nx // 2) * cols), pieces[0].dtype),
        name="assemble",
    )(pos, *pieces)


def layer(activations, grad_out, gate_pre, up_pre, gate_up, down_weight):
    tokens = activations.shape[0]
    slab, width = down_weight.shape
    nx, ny, nz = lax.axis_size(X), lax.axis_size(Y), lax.axis_size(ZH)
    dp_count = lax.axis_size(DP)
    rows = tokens // (ny * nz)
    xi, zi, ci = lax.axis_index(X), lax.axis_index(Z), lax.axis_index(C)
    yi = lax.axis_index(Y)
    pos = jnp.stack([zi, ci, xi, yi]).astype(jnp.int32)

    near, far = [down_weight], []
    far.append(swap(down_weight, Z))
    for _ in range(1, nx):
        near.append(ring(near[-1]))
        far.append(ring(far[-1]))
    gate_near = gate_up.reshape(slab, 2 * width)
    gate_far = [swap(gate_near, Z)]
    gate_near = [gate_near] + [None] * (nx - 1)
    gate_far = gate_far + [None] * (nx - 1)
    gate_near[1] = shift(gate_near[0], X, 1)
    gate_far[1] = shift(gate_far[0], X, -1)
    gate_near[3] = shift(gate_near[0], X, -1)
    gate_near[2] = shift(gate_near[1], X, 1)
    gate_far[3] = swap(gate_near[1], Z)
    gate_far[2] = swap(gate_near[2], Z)

    out_mine, out_theirs = to_columns(grad_out, pos, slab)
    out_theirs = swap(out_theirs, C)
    out_mine, _ = lax.optimization_barrier((out_mine, far[1]))
    out_all = jnp.concatenate([out_mine, out_theirs])
    both = jnp.concatenate([gate_pre.T, up_pre.T])
    other = swap(both, C)
    hidden, gate_factor, up_factor = factors(both, other)
    act_mine, act_theirs = to_columns(activations, pos, slab)
    act_theirs = swap(act_theirs, C)
    act_all = jnp.concatenate([act_mine, act_theirs])

    down = jnp.zeros((2 * nx, slab, width), BF)
    for h in range(nx):
        x = (xi + (2 * ci - 1) * h) & (nx - 1)
        down = lax.dynamic_update_slice(down, near[h][None], (zi * nx + x, 0, 0))
        down = lax.dynamic_update_slice(down, far[h][None], ((1 - zi) * nx + x, 0, 0))
    down = down.reshape(2 * nx * slab, width)
    part_h = lax.dot_general(down, out_all, (((0,), (1,)), ((), ())), preferred_element_type=F32)
    got_h = swap(part_h, C)
    grad_hidden = grad_hidden_of(part_h, got_h, gate_factor, up_factor)

    pieces = []
    for n in range(2):
        w = jnp.concatenate(
            [g[q] for q in (2 * n, 2 * n + 1) for g in (gate_near, gate_far)]
        )
        part = lax.dot_general(
            grad_hidden, w, (((0,), (1,)), ((), ())), preferred_element_type=F32
        ).astype(BF)
        if n == 0:
            part = part.reshape(2, ny * nz, rows, -1).transpose(1, 0, 2, 3)
            part = part.reshape(ny, 2 * nz * rows, -1)
            part = lax.all_to_all(part, Y, 0, 0, tiled=True)
            part = jnp.sum(part.astype(F32), axis=0)
        else:
            blocks = cut(part, pos, ny, nz, rows)
            part = blocks[0].astype(F32)
            for j in range(1, ny):
                got = shift(blocks[j], Y, j)
                part = part + got.astype(F32)
        part = part.astype(BF).reshape(nz, 2 * rows, -1)
        part = lax.all_to_all(part, ZH, 0, 0, tiled=True)
        part = jnp.sum(part.astype(F32), axis=0).astype(BF)
        got = swap(part[rows:], C)
        piece = from_slabs(part[:rows], got, pos, slab)
        piece = lax.all_gather(piece, ZH, axis=0, tiled=True)
        pieces.append(piece)
        for j in range(1, ny):
            pieces.append(shift(piece, Y, j))
    grad_input = assemble(pieces, pos, 2 * slab, nx, ny)

    grad_down = lax.dot_general(
        out_all, hidden, (((0,), (1,)), ((), ())), preferred_element_type=F32
    ).astype(BF)
    grad_down = lax.psum_scatter(grad_down, (Z, X), scatter_dimension=0, tiled=True)
    grad_down = grad_down.astype(F32) / dp_count
    total = lax.dot_general(
        act_all, grad_hidden, (((0,), (1,)), ((), ())), preferred_element_type=F32
    ).astype(BF)
    total = lax.psum_scatter(total, (Z, X), scatter_dimension=0, tiled=True)
    grad_gate_up = (total.astype(F32) / dp_count).reshape(slab, 2, width)
    return (grad_input, grad_gate_up, grad_down)


def solution(mesh):
    split = Mesh(
        mesh.devices.reshape(2, 4, 2, 4, 4), ("dp_0", "dp_1", "dp_2", "tensor_0", "tensor_1")
    )
    return jax.shard_map(
        layer,
        mesh=split,
        in_specs=(
            P(DP, None),
            P(DP, None),
            P(DP, TENSOR),
            P(DP, TENSOR),
            P(DP, None, TENSOR),
            P(DP, TENSOR),
        ),
        out_specs=(P(DP, None), P(DP, None, TENSOR), P(DP, TENSOR)),
        check_vma=False,
    )
```

```python
import functools

import jax
import jax.numpy as jnp
from jax import lax
from jax.experimental import pallas as pl
from jax.experimental.pallas import tpu as pltpu
from jax.sharding import Mesh
from jax.sharding import PartitionSpec as P

Z, X, C = "dp_0", "dp_1", "dp_2"
DP = (Z, X, C)
ZH, Y = "tensor_0", "tensor_1"
TENSOR = (ZH, Y)
BF = jnp.bfloat16
F32 = jnp.float32


def shift(v, axis, step):
    n = lax.axis_size(axis)
    return lax.ppermute(v, axis, [(i, (i + step) % n) for i in range(n)])


def swap(v, axis):
    return lax.ppermute(v, axis, [(0, 1), (1, 0)])


def to_columns_kernel(pos_ref, x_ref, mine_ref, theirs_ref, *, slab):
    for core in range(2):

        @pl.when(pos_ref[1] == core)
        def _(core=core):
            for k in range(x_ref.shape[1] // (2 * slab)):
                for ref, side in ((mine_ref, core), (theirs_ref, 1 - core)):
                    at = (2 * k + side) * slab
                    ref[:, k * slab : (k + 1) * slab] = x_ref[:, at : at + slab]


def to_columns(x, pos, slab):
    tokens, width = x.shape
    rows = 64
    out = jax.ShapeDtypeStruct((tokens, width // 2), x.dtype)
    return pl.pallas_call(
        functools.partial(to_columns_kernel, slab=slab),
        grid_spec=pltpu.PrefetchScalarGridSpec(
            num_scalar_prefetch=1,
            grid=(tokens // rows,),
            in_specs=[pl.BlockSpec((rows, width), lambda i, s: (i, 0))],
            out_specs=[pl.BlockSpec((rows, width // 2), lambda i, s: (i, 0))] * 2,
        ),
        out_shape=[out, out],
        name="to_columns",
    )(pos, x)


def factors_kernel(own_ref, other_ref, hidden_ref, gate_ref, up_ref):
    width = hidden_ref.shape[0]
    tokens = own_ref.shape[1]
    for a, ref in enumerate((own_ref, other_ref)):
        at = slice(a * tokens, (a + 1) * tokens)
        g = ref[:width].astype(F32)
        u = ref[width:].astype(F32)
        s = 1.0 / (1.0 + jnp.exp(-g))
        silu = g * s
        hidden_ref[:, at] = (silu * u).astype(BF)
        gate_ref[:, at] = u * s * (1.0 + g * (1.0 - s))
        up_ref[:, at] = silu


def factors(own, other):
    width, tokens = own.shape
    outs = [jax.ShapeDtypeStruct((width // 2, 2 * tokens), t) for t in (BF, F32, F32)]
    return pl.pallas_call(factors_kernel, out_shape=outs, name="factors")(own, other)


def grad_hidden_kernel(part_ref, got_ref, gate_ref, up_ref, o_ref):
    width, both = part_ref.shape
    tokens = both // 2
    for a in range(2):
        at = slice(a * tokens, (a + 1) * tokens)
        h = part_ref[:, at] + got_ref[:, tokens - a * tokens : both - a * tokens]
        o_ref[:width, at] = (h * gate_ref[:, at]).astype(BF)
        o_ref[width:, at] = (h * up_ref[:, at]).astype(BF)


def grad_hidden_of(part, got, gate, up):
    width, both = part.shape
    return pl.pallas_call(
        grad_hidden_kernel,
        out_shape=jax.ShapeDtypeStruct((2 * width, both), BF),
        name="grad_hidden",
    )(part, got, gate, up)


def cut_kernel(pos_ref, x_ref, *o_refs):
    n = len(o_refs)
    for j, o_ref in enumerate(o_refs):
        at = (pos_ref[3] + j) & (n - 1)
        for a in range(2):
            o_ref[:, a] = x_ref[a, at]


def cut(x, pos, n, m, rows):
    cols = x.shape[1]
    out = jax.ShapeDtypeStruct((m, 2, rows, cols), x.dtype)
    outs = pl.pallas_call(
        cut_kernel,
        in_specs=[
            pl.BlockSpec(memory_space=pltpu.SMEM),
            pl.BlockSpec(memory_space=pltpu.VMEM),
        ],
        out_shape=[out] * n,
        name="cut",
    )(pos, x.reshape(2, n, m, rows, cols))
    return [o.reshape(m * 2 * rows, cols) for o in outs]


def from_slabs_kernel(pos_ref, own_ref, other_ref, o_ref, *, slab):
    core_odd = pos_ref[1] == 1
    own, other = own_ref[...], other_ref[...]
    for i in range(own.shape[1] // slab):
        mine, theirs = (v[:, i * slab : (i + 1) * slab] for v in (own, other))
        even = jnp.where(core_odd, theirs, mine)
        odd = jnp.where(core_odd, mine, theirs)
        both = jnp.concatenate([even, odd], axis=1)
        o_ref[:, 2 * i * slab : 2 * (i + 1) * slab] = both


def from_slabs(own, other, pos, slab):
    rows, cols = own.shape
    vmem = pl.BlockSpec(memory_space=pltpu.VMEM)
    return pl.pallas_call(
        functools.partial(from_slabs_kernel, slab=slab),
        in_specs=[pl.BlockSpec(memory_space=pltpu.SMEM), vmem, vmem],
        out_shape=jax.ShapeDtypeStruct((rows, 2 * cols), own.dtype),
        name="from_slabs",
    )(pos, own, other)


def assemble_kernel(pos_ref, *refs, block, nx, ny):
    o_ref = refs[-1]
    zi, xi, yi = pos_ref[0], pos_ref[2], pos_ref[3]
    rows = refs[0].shape[0]
    for n in range(nx // 2):
        for j in range(ny):
            ref = refs[n * ny + j]
            row = pl.multiple_of(((yi - j) & (ny - 1)) * rows, rows)
            for i in range(2):
                q = 2 * n + i
                for d, at in enumerate((zi * nx + ((xi - q) & (nx - 1)), (1 - zi) * nx + ((xi + q) & (nx - 1)))):
                    src = (2 * i + d) * block
                    o_ref[pl.ds(row, rows), pl.ds(pl.multiple_of(at * block, 128), block)] = ref[
                        :, src : src + block
                    ]


def assemble(pieces, pos, block, nx, ny):
    rows, cols = pieces[0].shape
    vmem = pl.BlockSpec(memory_space=pltpu.VMEM)
    return pl.pallas_call(
        functools.partial(assemble_kernel, block=block, nx=nx, ny=ny),
        in_specs=[pl.BlockSpec(memory_space=pltpu.SMEM)] + [vmem] * len(pieces),
        out_shape=jax.ShapeDtypeStruct((ny * rows, (nx // 2) * cols), pieces[0].dtype),
        name="assemble",
    )(pos, *pieces)


def layer(activations, grad_out, gate_pre, up_pre, gate_up, down_weight):
    tokens = activations.shape[0]
    slab, width = down_weight.shape
    nx, ny, nz = lax.axis_size(X), lax.axis_size(Y), lax.axis_size(ZH)
    dp_count = lax.axis_size(DP)
    rows = tokens // (ny * nz)
    xi, zi, ci = lax.axis_index(X), lax.axis_index(Z), lax.axis_index(C)
    yi = lax.axis_index(Y)
    pos = jnp.stack([zi, ci, xi, yi]).astype(jnp.int32)

    near, far = [down_weight] + [None] * (nx - 1), [None] * nx
    far[0] = swap(down_weight, Z)
    near[1] = shift(near[0], X, 1)
    near[3] = shift(near[0], X, -1)
    far[1] = shift(far[0], X, -1)
    far[3] = shift(far[0], X, 1)
    near[2] = shift(near[1], X, 1)
    far[2] = shift(far[1], X, -1)
    gate_near = gate_up.reshape(slab, 2 * width)
    gate_far = [swap(gate_near, Z)]
    gate_near = [gate_near] + [None] * (nx - 1)
    gate_far = gate_far + [None] * (nx - 1)
    gate_near[1] = shift(gate_near[0], X, 1)
    gate_far[1] = shift(gate_far[0], X, -1)
    gate_near[3] = shift(gate_near[0], X, -1)
    gate_near[2] = shift(gate_near[1], X, 1)
    gate_far[3] = swap(gate_near[1], Z)
    gate_far[2] = swap(gate_near[2], Z)

    out_mine, out_theirs = to_columns(grad_out, pos, slab)
    out_theirs = swap(out_theirs, C)
    out_mine, _ = lax.optimization_barrier((out_mine, far[1]))
    out_all = jnp.concatenate([out_mine, out_theirs])
    both = jnp.concatenate([gate_pre.T, up_pre.T])
    other = swap(both, C)
    hidden, gate_factor, up_factor = factors(both, other)
    act_mine, act_theirs = to_columns(activations, pos, slab)
    act_theirs = swap(act_theirs, C)
    act_all = jnp.concatenate([act_mine, act_theirs])

    down = jnp.zeros((2 * nx, slab, width), BF)
    for h in (0, 1, 3, 2):
        x = (xi - h) & (nx - 1)
        down = lax.dynamic_update_slice(down, near[h][None], (zi * nx + x, 0, 0))
        x = (xi + h) & (nx - 1)
        down = lax.dynamic_update_slice(down, far[h][None], ((1 - zi) * nx + x, 0, 0))
    down = down.reshape(2 * nx * slab, width)
    part_h = lax.dot_general(down, out_all, (((0,), (1,)), ((), ())), preferred_element_type=F32)
    got_h = swap(part_h, C)
    grad_hidden = grad_hidden_of(part_h, got_h, gate_factor, up_factor)

    pieces = []
    for n in range(2):
        w = jnp.concatenate(
            [g[q] for q in (2 * n, 2 * n + 1) for g in (gate_near, gate_far)]
        )
        part = lax.dot_general(
            grad_hidden, w, (((0,), (1,)), ((), ())), preferred_element_type=F32
        ).astype(BF)
        if n == 0:
            part = part.reshape(2, ny * nz, rows, -1).transpose(1, 0, 2, 3)
            part = part.reshape(ny, 2 * nz * rows, -1)
            part = lax.all_to_all(part, Y, 0, 0, tiled=True)
            part = jnp.sum(part.astype(F32), axis=0)
        else:
            blocks = cut(part, pos, ny, nz, rows)
            part = blocks[0].astype(F32)
            for j in range(1, ny):
                got = shift(blocks[j], Y, j)
                part = part + got.astype(F32)
        part = part.astype(BF).reshape(nz, 2 * rows, -1)
        part = lax.all_to_all(part, ZH, 0, 0, tiled=True)
        part = jnp.sum(part.astype(F32), axis=0).astype(BF)
        got = swap(part[rows:], C)
        piece = from_slabs(part[:rows], got, pos, slab)
        piece = lax.all_gather(piece, ZH, axis=0, tiled=True)
        pieces.append(piece)
        for j in range(1, ny):
            pieces.append(shift(piece, Y, j))
    grad_input = assemble(pieces, pos, 2 * slab, nx, ny)

    grad_down = lax.dot_general(
        out_all, hidden, (((0,), (1,)), ((), ())), preferred_element_type=F32
    ).astype(BF)
    grad_down = lax.psum_scatter(grad_down, (Z, X), scatter_dimension=0, tiled=True)
    grad_down = grad_down.astype(F32) / dp_count
    total = lax.dot_general(
        act_all, grad_hidden, (((0,), (1,)), ((), ())), preferred_element_type=F32
    ).astype(BF)
    total = lax.psum_scatter(total, (Z, X), scatter_dimension=0, tiled=True)
    grad_gate_up = (total.astype(F32) / dp_count).reshape(slab, 2, width)
    return (grad_input, grad_gate_up, grad_down)


def solution(mesh):
    split = Mesh(
        mesh.devices.reshape(2, 4, 2, 4, 4), ("dp_0", "dp_1", "dp_2", "tensor_0", "tensor_1")
    )
    return jax.shard_map(
        layer,
        mesh=split,
        in_specs=(
            P(DP, None),
            P(DP, None),
            P(DP, TENSOR),
            P(DP, TENSOR),
            P(DP, None, TENSOR),
            P(DP, TENSOR),
        ),
        out_specs=(P(DP, None), P(DP, None, TENSOR), P(DP, TENSOR)),
        check_vma=False,
    )
```

```python
import functools

import jax
import jax.numpy as jnp
from jax import lax
from jax.experimental import pallas as pl
from jax.experimental.pallas import tpu as pltpu
from jax.sharding import Mesh
from jax.sharding import PartitionSpec as P

Z, X, C = "dp_0", "dp_1", "dp_2"
DP = (Z, X, C)
ZH, Y = "tensor_0", "tensor_1"
TENSOR = (ZH, Y)
BF = jnp.bfloat16
F32 = jnp.float32


def shift(v, axis, step):
    n = lax.axis_size(axis)
    return lax.ppermute(v, axis, [(i, (i + step) % n) for i in range(n)])


def swap(v, axis):
    return lax.ppermute(v, axis, [(0, 1), (1, 0)])


def to_columns_kernel(pos_ref, x_ref, mine_ref, theirs_ref, *, slab):
    for core in range(2):

        @pl.when(pos_ref[1] == core)
        def _(core=core):
            for k in range(x_ref.shape[1] // (2 * slab)):
                for ref, side in ((mine_ref, core), (theirs_ref, 1 - core)):
                    at = (2 * k + side) * slab
                    ref[:, k * slab : (k + 1) * slab] = x_ref[:, at : at + slab]


def to_columns(x, pos, slab):
    tokens, width = x.shape
    rows = 64
    out = jax.ShapeDtypeStruct((tokens, width // 2), x.dtype)
    return pl.pallas_call(
        functools.partial(to_columns_kernel, slab=slab),
        grid_spec=pltpu.PrefetchScalarGridSpec(
            num_scalar_prefetch=1,
            grid=(tokens // rows,),
            in_specs=[pl.BlockSpec((rows, width), lambda i, s: (i, 0))],
            out_specs=[pl.BlockSpec((rows, width // 2), lambda i, s: (i, 0))] * 2,
        ),
        out_shape=[out, out],
        name="to_columns",
    )(pos, x)


def factors_kernel(own_ref, other_ref, hidden_ref, gate_ref, up_ref):
    width = hidden_ref.shape[0]
    tokens = own_ref.shape[1]
    for a, ref in enumerate((own_ref, other_ref)):
        at = slice(a * tokens, (a + 1) * tokens)
        g = ref[:width].astype(F32)
        u = ref[width:].astype(F32)
        s = 1.0 / (1.0 + jnp.exp(-g))
        silu = g * s
        hidden_ref[:, at] = (silu * u).astype(BF)
        gate_ref[:, at] = u * s * (1.0 + g * (1.0 - s))
        up_ref[:, at] = silu


def factors(own, other):
    width, tokens = own.shape
    outs = [jax.ShapeDtypeStruct((width // 2, 2 * tokens), t) for t in (BF, F32, F32)]
    return pl.pallas_call(factors_kernel, out_shape=outs, name="factors")(own, other)


def grad_hidden_kernel(part_ref, got_ref, gate_ref, up_ref, o_ref):
    width, both = part_ref.shape
    tokens = both // 2
    for a in range(2):
        at = slice(a * tokens, (a + 1) * tokens)
        h = part_ref[:, at] + got_ref[:, tokens - a * tokens : both - a * tokens]
        o_ref[:width, at] = (h * gate_ref[:, at]).astype(BF)
        o_ref[width:, at] = (h * up_ref[:, at]).astype(BF)


def grad_hidden_of(part, got, gate, up):
    width, both = part.shape
    return pl.pallas_call(
        grad_hidden_kernel,
        out_shape=jax.ShapeDtypeStruct((2 * width, both), BF),
        name="grad_hidden",
    )(part, got, gate, up)


def cut_kernel(pos_ref, x_ref, *o_refs):
    n = len(o_refs)
    for j, o_ref in enumerate(o_refs):
        at = (pos_ref[3] + j) & (n - 1)
        for a in range(2):
            o_ref[:, a] = x_ref[a, at]


def cut(x, pos, n, m, rows):
    cols = x.shape[1]
    out = jax.ShapeDtypeStruct((m, 2, rows, cols), x.dtype)
    outs = pl.pallas_call(
        cut_kernel,
        in_specs=[
            pl.BlockSpec(memory_space=pltpu.SMEM),
            pl.BlockSpec(memory_space=pltpu.VMEM),
        ],
        out_shape=[out] * n,
        name="cut",
    )(pos, x.reshape(2, n, m, rows, cols))
    return [o.reshape(m * 2 * rows, cols) for o in outs]


def from_slabs_kernel(pos_ref, own_ref, other_ref, o_ref, *, slab):
    core_odd = pos_ref[1] == 1
    own, other = own_ref[...], other_ref[...]
    for i in range(own.shape[1] // slab):
        mine, theirs = (v[:, i * slab : (i + 1) * slab] for v in (own, other))
        even = jnp.where(core_odd, theirs, mine)
        odd = jnp.where(core_odd, mine, theirs)
        both = jnp.concatenate([even, odd], axis=1)
        o_ref[:, 2 * i * slab : 2 * (i + 1) * slab] = both


def from_slabs(own, other, pos, slab):
    rows, cols = own.shape
    vmem = pl.BlockSpec(memory_space=pltpu.VMEM)
    return pl.pallas_call(
        functools.partial(from_slabs_kernel, slab=slab),
        in_specs=[pl.BlockSpec(memory_space=pltpu.SMEM), vmem, vmem],
        out_shape=jax.ShapeDtypeStruct((rows, 2 * cols), own.dtype),
        name="from_slabs",
    )(pos, own, other)


def assemble_kernel(pos_ref, *refs, block, nx, ny):
    o_ref = refs[-1]
    zi, xi, yi = pos_ref[0], pos_ref[2], pos_ref[3]
    rows = refs[0].shape[0]
    for n in range(nx // 2):
        for j in range(ny):
            ref = refs[n * ny + j]
            row = pl.multiple_of(((yi - j) & (ny - 1)) * rows, rows)
            for i in range(2):
                q = 2 * n + i
                for d, at in enumerate((zi * nx + ((xi - q) & (nx - 1)), (1 - zi) * nx + ((xi + q) & (nx - 1)))):
                    src = (2 * i + d) * block
                    o_ref[pl.ds(row, rows), pl.ds(pl.multiple_of(at * block, 128), block)] = ref[
                        :, src : src + block
                    ]


def assemble(pieces, pos, block, nx, ny):
    rows, cols = pieces[0].shape
    vmem = pl.BlockSpec(memory_space=pltpu.VMEM)
    return pl.pallas_call(
        functools.partial(assemble_kernel, block=block, nx=nx, ny=ny),
        in_specs=[pl.BlockSpec(memory_space=pltpu.SMEM)] + [vmem] * len(pieces),
        out_shape=jax.ShapeDtypeStruct((ny * rows, (nx // 2) * cols), pieces[0].dtype),
        name="assemble",
    )(pos, *pieces)


def layer(activations, grad_out, gate_pre, up_pre, gate_up, down_weight):
    tokens = activations.shape[0]
    slab, width = down_weight.shape
    nx, ny, nz = lax.axis_size(X), lax.axis_size(Y), lax.axis_size(ZH)
    dp_count = lax.axis_size(DP)
    rows = tokens // (ny * nz)
    xi, zi, ci = lax.axis_index(X), lax.axis_index(Z), lax.axis_index(C)
    yi = lax.axis_index(Y)
    pos = jnp.stack([zi, ci, xi, yi]).astype(jnp.int32)

    near, far = [down_weight] + [None] * (nx - 1), [None] * nx
    far[0] = swap(down_weight, Z)
    near[1] = shift(near[0], X, 1)
    near[3] = shift(near[0], X, -1)
    far[1] = shift(far[0], X, -1)
    far[3] = shift(far[0], X, 1)
    near[2] = shift(near[1], X, 1)
    far[2] = shift(far[1], X, -1)
    gate_near = gate_up.reshape(slab, 2 * width)
    gate_far = [swap(gate_near, Z)]
    gate_near = [gate_near] + [None] * (nx - 1)
    gate_far = gate_far + [None] * (nx - 1)
    gate_near[1] = shift(gate_near[0], X, 1)
    gate_far[1] = shift(gate_far[0], X, -1)
    gate_near[3] = shift(gate_near[0], X, -1)
    gate_near[2] = shift(gate_near[1], X, 1)
    gate_far[3] = swap(gate_near[1], Z)
    gate_far[2] = shift(gate_far[1], X, -1)

    out_mine, out_theirs = to_columns(grad_out, pos, slab)
    out_theirs = swap(out_theirs, C)
    out_mine, _ = lax.optimization_barrier((out_mine, far[1]))
    out_all = jnp.concatenate([out_mine, out_theirs])
    both = jnp.concatenate([gate_pre.T, up_pre.T])
    other = swap(both, C)
    hidden, gate_factor, up_factor = factors(both, other)
    act_mine, act_theirs = to_columns(activations, pos, slab)
    act_theirs = swap(act_theirs, C)
    act_all = jnp.concatenate([act_mine, act_theirs])

    down = jnp.zeros((2 * nx, slab, width), BF)
    for h in (0, 1, 3):
        x = (xi - h) & (nx - 1)
        down = lax.dynamic_update_slice(down, near[h][None], (zi * nx + x, 0, 0))
        x = (xi + h) & (nx - 1)
        down = lax.dynamic_update_slice(down, far[h][None], ((1 - zi) * nx + x, 0, 0))
    x = (xi + 2) & (nx - 1)
    down = lax.dynamic_update_slice(down, near[2][None], (zi * nx + x, 0, 0))
    down = lax.dynamic_update_slice(down, far[2][None], ((1 - zi) * nx + x, 0, 0))
    down = down.reshape(2 * nx * slab, width)
    part_h = lax.dot_general(down, out_all, (((0,), (1,)), ((), ())), preferred_element_type=F32)
    got_h = swap(part_h, C)
    grad_hidden = grad_hidden_of(part_h, got_h, gate_factor, up_factor)

    pieces = []
    for n in range(2):
        w = jnp.concatenate(
            [g[q] for q in (2 * n, 2 * n + 1) for g in (gate_near, gate_far)]
        )
        part = lax.dot_general(
            grad_hidden, w, (((0,), (1,)), ((), ())), preferred_element_type=F32
        ).astype(BF)
        if n == 0:
            part = part.reshape(2, ny * nz, rows, -1).transpose(1, 0, 2, 3)
            part = part.reshape(ny, 2 * nz * rows, -1)
            part = lax.all_to_all(part, Y, 0, 0, tiled=True)
            part = jnp.sum(part.astype(F32), axis=0)
        else:
            blocks = cut(part, pos, ny, nz, rows)
            part = blocks[0].astype(F32)
            for j in range(1, ny):
                got = shift(blocks[j], Y, j)
                part = part + got.astype(F32)
        part = part.astype(BF).reshape(nz, 2 * rows, -1)
        part = lax.all_to_all(part, ZH, 0, 0, tiled=True)
        part = jnp.sum(part.astype(F32), axis=0).astype(BF)
        got = swap(part[rows:], C)
        piece = from_slabs(part[:rows], got, pos, slab)
        piece = lax.all_gather(piece, ZH, axis=0, tiled=True)
        pieces.append(piece)
        for j in range(1, ny):
            pieces.append(shift(piece, Y, j))
    grad_input = assemble(pieces, pos, 2 * slab, nx, ny)

    grad_down = lax.dot_general(
        out_all, hidden, (((0,), (1,)), ((), ())), preferred_element_type=F32
    ).astype(BF)
    grad_down = lax.psum_scatter(grad_down, (Z, X), scatter_dimension=0, tiled=True)
    grad_down = grad_down.astype(F32) / dp_count
    total = lax.dot_general(
        act_all, grad_hidden, (((0,), (1,)), ((), ())), preferred_element_type=F32
    ).astype(BF)
    total = lax.psum_scatter(total, (Z, X), scatter_dimension=0, tiled=True)
    grad_gate_up = (total.astype(F32) / dp_count).reshape(slab, 2, width)
    return (grad_input, grad_gate_up, grad_down)


def solution(mesh):
    split = Mesh(
        mesh.devices.reshape(2, 4, 2, 4, 4), ("dp_0", "dp_1", "dp_2", "tensor_0", "tensor_1")
    )
    return jax.shard_map(
        layer,
        mesh=split,
        in_specs=(
            P(DP, None),
            P(DP, None),
            P(DP, TENSOR),
            P(DP, TENSOR),
            P(DP, None, TENSOR),
            P(DP, TENSOR),
        ),
        out_specs=(P(DP, None), P(DP, None, TENSOR), P(DP, TENSOR)),
        check_vma=False,
    )
```
